256 devices in a mesh: dp: 16 (over y_hi, x, core), mp: 16 (over z, y_lo).
Axes of the slice: x: 4, y: 4 (y_hi: 2, y_lo: 2; y = y_hi * 2 + y_lo), z: 8, core: 2. Of those that a mesh axis runs over, the one named last changes fastest.
Arguments:
- tokens: bfloat16 [8192, 8192], P(('dp', 'mp')), parts along dimension 0, may hold values from -6 to 6
- norm_gain: float32 [8192], replicated, may hold values from 0.5 to 1.5
- qkv_weight: bfloat16 [8192, 10240], P(None, 'mp'), may hold values from -0.0625 to 0.0625
- qkv_bias: float32 [10240], P('mp'), may hold values from -3 to 3
- qkv_grad: bfloat16 [8192, 10240], P('dp', 'mp'), parts along dimension 0, may hold values from -6 to 6
Outputs:
- qkv: bfloat16 [8192, 10240], P('dp', 'mp'), parts along dimension 0
- tokens_grad: float32 [8192, 8192], P(('dp', 'mp')), parts along dimension 0
- gain_grad: float32 [131072], P('dp'), parts along dimension 0
- bias_grad: float32 [163840], P(('dp', 'mp')), parts along dimension 0
The draws below stay inside these ranges and needn't reach their ends.
There are 16 independent parts, one for each index of `dp`. The reference program is written for one: setup_inputs(seed, part) draws one part's arguments, and reference() takes and returns one part's arrays. A program takes and returns all parts, laid end to end along the dimension named above; an argument that names none is the same for every part. Nothing has to cross between parts.
All inputs are finite; a program needn't handle non-finite values.
Results may differ from the reference program's by a relative error of at most 0.0046.
Values may be sent and summed in bfloat16 or wider, within the bound.
A program may use at most 128 MiB of HBM per device.

```python
import jax
import jax.numpy as jnp
from jax import lax

D = 8192
HEAD_DIM = 128
GROUP = 10
COLS = 10240
STRIDE = 2048
TOK_DEV = 32
TOKENS = 512


def strengthened(values, own_key, source, target, shards_of, factor):
    def block_of(axis_at):
        return (jnp.arange(values.shape[axis_at]) // (values.shape[axis_at] // shards_of)).reshape((-1,) + (1,) * (values.ndim - 1 - axis_at))

    first = jax.random.permutation(own_key, shards_of)[block_of(target)]
    far = (block_of(target) + shards_of // 2) % shards_of
    return jnp.where((block_of(source) == first) | (block_of(source) == far), factor * values, values)


def shard_levels(stream_key, shape, cuts, smallest, top_value):
    def one(axis_at, blocks):
        heights = jax.random.uniform(jax.random.fold_in(jax.random.fold_in(stream_key, 6), axis_at), (blocks,), jnp.float32, smallest / len(cuts), top_value / len(cuts))
        return jnp.repeat(jnp.exp(heights), shape[axis_at] // blocks).reshape((-1,) + (1,) * (len(shape) - axis_at - 1))

    factor_of = one(*cuts[0])
    for cut in cuts[1:]:
        factor_of = factor_of * one(*cut)
    return factor_of


def gaussian(own_key, dims, deviation, bound, shards=(), kind=jnp.bfloat16):
    array = deviation * jax.random.normal(own_key, dims, jnp.float32)
    if shards:
        array = array * shard_levels(own_key, dims, shards, -0.22, 0.18)
    return jnp.clip(array, -bound, bound).astype(kind)


def gaussian_with(stream_key, extent, deviation, limit, cuts, heavy, kind=jnp.bfloat16):
    array = deviation * jax.random.normal(stream_key, extent, jnp.float32)
    if cuts:
        array = array * shard_levels(stream_key, extent, cuts, -0.22, 0.18)
    return jnp.clip(strengthened(array, jax.random.fold_in(stream_key, 3), *heavy), -limit, limit).astype(kind)


def setup_inputs(seed: int = 0, part: int = 0) -> dict:
    key_list = jax.random.split(jax.random.key(seed), 6)
    part_keys = jax.random.split(jax.random.fold_in(key_list[5], part), 6)
    return {
        "tokens": gaussian(part_keys[0], (TOKENS, D), 1.0, 6.0, ((0, 16),)),
        "norm_gain": jnp.clip(1.0 + 0.1 * jax.random.normal(key_list[1], (D,), jnp.float32), 0.5, 1.5),
        "qkv_weight": gaussian(key_list[2], (D, COLS), D ** -0.5, 0.0625, ((1, 16),)),
        "qkv_bias": gaussian(key_list[3], (COLS,), 0.5, 3.0, ((0, 16),), jnp.float32),
        "qkv_grad": gaussian_with(part_keys[4], (TOKENS, COLS), 1.0, 6.0, ((1, 16),), (1, 0, 16, 2.0)),
    }


def rotate_heads(joined, first_col, position, sign):
    rows, cols = joined.shape
    heads = cols // HEAD_DIM
    half = HEAD_DIM // 2
    parts = joined.reshape(rows, heads, 2, half)
    inverse = jnp.exp(-jnp.log(jnp.float32(1000000.0)) * (2.0 * jnp.arange(half).astype(jnp.float32) / HEAD_DIM))
    angle = position.astype(jnp.float32)[:, None] * inverse[None, :]
    cosine = jnp.cos(angle)[:, None, :]
    sine = sign * jnp.sin(angle)[:, None, :]
    first = parts[:, :, 0, :]
    second = parts[:, :, 1, :]
    turned = jnp.stack([first * cosine - second * sine, second * cosine + first * sine], axis=2)
    head_index = first_col // HEAD_DIM + jnp.arange(heads)
    rotated = head_index % GROUP != GROUP - 1
    result = jnp.where(rotated[None, :, None, None], turned, parts)
    return result.reshape(rows, cols)

def reference(tokens, norm_gain, qkv_weight, qkv_bias, qkv_grad):
    row_index = jnp.arange(TOKENS).astype(jnp.int32)
    position = row_index // TOK_DEV * STRIDE + row_index % TOK_DEV
    values = tokens.astype(jnp.float32)
    scale = lax.rsqrt(lax.optimization_barrier(jnp.mean(values * values, axis=1, keepdims=True)) + 1e-06)
    normed = (values * scale * norm_gain[None, :]).astype(jnp.bfloat16)
    joined = jnp.dot(normed, qkv_weight, preferred_element_type=jnp.float32) + qkv_bias[None, :]
    qkv = rotate_heads(joined, 0, position, 1.0).astype(jnp.bfloat16)
    joined_grad = rotate_heads(qkv_grad.astype(jnp.float32), 0, position, -1.0)
    bias_grad = lax.optimization_barrier(jnp.sum(joined_grad, axis=0))
    joined_low = joined_grad.astype(jnp.bfloat16)
    normed_grad = lax.dot_general(joined_low, qkv_weight, (((1,), (1,)), ((), ())), preferred_element_type=jnp.float32)
    gain_grad = lax.optimization_barrier(jnp.sum(normed_grad * values * scale, axis=0))
    inner = lax.optimization_barrier(jnp.mean(norm_gain[None, :] * normed_grad * values, axis=1, keepdims=True))
    tokens_grad = scale * norm_gain[None, :] * normed_grad - values * scale * scale * scale * inner
    return (qkv, tokens_grad, gain_grad, bias_grad)
```

```python
import functools

import jax
import jax.numpy as jnp
import numpy as np
from jax import lax
from jax.experimental import pallas as pl
from jax.experimental.pallas import tpu as pltpu
from jax.sharding import Mesh
from jax.sharding import PartitionSpec as P

HEAD = 128
SEQ_LEN = 32768
MESH = pl.DeviceIdType.MESH
AXES = ("yh", "x", "core", "z", "yl")
Z = 8
N = 8
PER = 7
f32 = jnp.float32
bf16 = jnp.bfloat16


def rcopy(src, dst, ssem, rsem, **where):
    return pltpu.make_async_remote_copy(
        src_ref=src, dst_ref=dst, send_sem=ssem, recv_sem=rsem, device_id=where, device_id_type=MESH
    )


def kernel(
    tok_h, w_h, qg_h, gain_h, bias_h, cos_h, sin_h,
    qkv_o, tg_o, gg_o, bg_o,
    w, tok, nrm, part, rb, sb, qb, qp, jl, out, ng, scl, inner, acc,
    gp, gr, gs, gy, gf, gain, bias, bgv, cosv, sinv,
    ag_r, ag_s, w_r, w_s, d_r, d_s, rs_r, rs_s, q_r, q_s, b_r, b_s, o_r, o_s,
    g_r, g_s, gy_r, gy_s, gf_r, gf_s, loc,
):
    rows, dim = tok_h.shape
    width = w_h.shape[1]
    F = dim // N
    H = F // 2
    half = dim // 2
    yh, core, z, yl = (lax.axis_index(a) for a in ("yh", "core", "z", "yl"))

    def zz(k):
        return lax.rem(z + (k + Z), Z)

    direct = {"yl": 1 - yl}
    other = {"yh": 1 - yh, "yl": 1 - yl}
    sibling = {"core": 1 - core}
    own = pl.ds(pl.multiple_of(yl * width, 128), width)
    far = pl.ds(pl.multiple_of((1 - yl) * width, 128), width)

    local = [
        pltpu.make_async_copy(tok_h, tok.at[z], loc.at[0]),
        pltpu.make_async_copy(qg_h, qb, loc.at[1]),
        pltpu.make_async_copy(cos_h, cosv, loc.at[2]),
        pltpu.make_async_copy(sin_h, sinv, loc.at[3]),
        pltpu.make_async_copy(gain_h, gain, loc.at[4]),
        pltpu.make_async_copy(bias_h, bias.at[:, own], loc.at[5]),
        pltpu.make_async_copy(w_h, w.at[:, own], loc.at[6]),
    ]
    for copy in local:
        copy.start()

    barrier = pltpu.get_barrier_semaphore()
    for k in range(1, Z):
        pl.semaphore_signal(barrier, inc=1, device_id={"z": zz(k)}, device_id_type=MESH)
    for where in (direct, other, sibling):
        pl.semaphore_signal(barrier, inc=1, device_id=where, device_id_type=MESH)
    pl.semaphore_wait(barrier, Z + 2)

    def ag_half(d, k):
        return d if k % 2 == 0 else 1 - d

    def ag_copy(d, k):
        step = k // 2
        block = zz(-step) if d == 0 else zz(step)
        cols = pl.ds(ag_half(d, k) * half, half)
        src = tok_h.at[:, cols] if step == 0 else tok.at[block, :, cols]
        return rcopy(src, tok.at[block, :, cols], ag_s.at[d, k], ag_r.at[d, k], z=zz(1 if d == 0 else -1))

    for k in range(2):
        for d in range(2):
            ag_copy(d, k).start()

    q_copy = rcopy(qg_h.at[:, 1 - yl], qp, q_s.at[0], q_r.at[0], **direct)
    q_copy.start()
    b_copy = rcopy(bias_h, bias.at[:, own], b_s.at[0], b_r.at[0], **direct)
    b_copy.start()

    share = F // 2
    piece = share // 2

    def w_copy(j, s):
        at = pl.ds(pl.multiple_of(j * F + core * share + s * piece, piece), piece)
        return rcopy(w_h.at[at], w.at[at, own], w_s.at[s, j], w_r.at[s, j], **(direct if s == 0 else other))

    def w_got(j, s):
        at = pl.ds(pl.multiple_of(j * F + core * share + s * piece, piece), piece)
        return rcopy(w.at[at, far], w.at[at, far], w_s.at[s, j], w_r.at[s, j], **(direct if s == 0 else other))

    def d_copy(j):
        at = pl.ds(pl.multiple_of(j * F + core * share, share), share)
        return rcopy(w.at[at, far], w.at[at, far], d_s.at[j], d_r.at[j], **sibling)

    def d_got(j):
        at = pl.ds(pl.multiple_of(j * F + (1 - core) * share, share), share)
        return rcopy(w.at[at, far], w.at[at, far], d_s.at[j], d_r.at[j], **sibling)

    def hand_on(j):
        w_got(j, 0).wait_recv()
        w_got(j, 1).wait_recv()
        d_copy(j).start()

    for j in range(N):
        w_copy(j, 0).start()
        w_copy(j, 1).start()

    def norm_block(b):
        step = min(512, dim)

        def sq(i, total):
            v = tok[b, :, pl.ds(pl.multiple_of(i * step, step), step)].astype(f32)
            v = v * v
            for q in range(step // 128):
                total = total + v[:, q * 128:(q + 1) * 128]
            return total

        total = lax.fori_loop(0, dim // step, sq, jnp.zeros((rows, 128), f32))
        mean = jnp.sum(total, axis=1, keepdims=True) / dim
        s = jnp.broadcast_to(lax.rsqrt(mean + 1e-06), (rows, 128))
        scl[b] = s
        wide = jnp.concatenate([s] * (step // 128), axis=1)

        def put(i, carry):
            at = pl.ds(pl.multiple_of(i * step, step), step)
            v = tok[b, :, at].astype(f32)
            nrm[b, :, at] = (v * wide * gain[:, at]).astype(bf16)
            return carry

        lax.fori_loop(0, dim // step, put, 0)

    def turn_back(x, line, b, is_value):
        c = cosv[line, pl.ds(pl.multiple_of(b * rows, rows), rows), :]
        s = sinv[line, pl.ds(pl.multiple_of(b * rows, rows), rows), :]
        r = x * c - pltpu.roll(x, HEAD // 2, 1) * s
        return r if is_value is None else jnp.where(is_value, x, r)

    heads = width // HEAD

    def own_columns():
        bgv[...] = jnp.zeros_like(bgv)

        def one(b, carry):
            at = pl.ds(pl.multiple_of(b * rows, rows), rows)
            for h in range(heads):
                value = (yl == 1) if h == heads - 1 else None
                hs = pl.ds(h * HEAD, HEAD)
                for line in range(2):
                    r = turn_back(qb[b, line, :, hs].astype(f32), line, b, value)
                    bgv[:, hs] += jnp.sum(r, axis=0, keepdims=True)
                r = turn_back(qb[b, yl, :, hs].astype(f32), yl, b, value)
                jl[at, pl.ds(pl.multiple_of(yl * width + h * HEAD, HEAD), HEAD)] = r.astype(bf16)
            return carry

        lax.fori_loop(0, Z, one, 0)

    def far_columns():
        def one(b, carry):
            at = pl.ds(pl.multiple_of(b * rows, rows), rows)
            for h in range(heads):
                value = (yl == 0) if h == heads - 1 else None
                r = turn_back(qp[b, :, pl.ds(h * HEAD, HEAD)].astype(f32), yl, b, value)
                jl[at, pl.ds(pl.multiple_of((1 - yl) * width + h * HEAD, HEAD), HEAD)] = r.astype(bf16)
            return carry

        lax.fori_loop(0, Z, one, 0)

    for k in range(1, 5):
        local[k].wait()
    own_columns()
    local[0].wait()
    norm_block(z)
    local[5].wait()
    bg_copy = pltpu.make_async_copy(bgv, bg_o, loc.at[7])
    bg_copy.start()

    for k in range(PER):
        for d in range(2):
            block = zz(-1 - k // 2) if d == 0 else zz(1 + k // 2)
            cols = pl.ds(ag_half(d, k) * half, half)
            spot = tok.at[block, :, cols]
            rcopy(spot, spot, ag_s.at[d, k], ag_r.at[d, k], z=z).wait_recv()
            if k + 2 < PER:
                ag_copy(d, k + 2).start()
        if k == 1:
            q_copy.wait_recv()
            b_copy.wait_recv()
            far_columns()
        if k % 2 == 1:
            norm_block(zz(-1 - k // 2))
            norm_block(zz(1 + k // 2))
        if k == 6:
            norm_block(zz(4))
        if 4 <= k:
            hand_on(k - 4)
    local[6].wait()

    bt = min(256, F)

    def backward_chunk(c):
        @pl.when(c < 6)
        def _():
            d_got(c).wait_recv()

        def one(t, carry):
            at = pl.ds(pl.multiple_of(c * F + t * bt, bt), bt)
            got = lax.dot_general(jl[...], w[at, :], (((1,), (1,)), ((), ())), preferred_element_type=f32)
            part[:, :, at] = got.reshape(Z, rows, bt)
            return carry

        lax.fori_loop(0, F // bt, one, 0)

    def span(c, hf):
        return pl.ds(pl.multiple_of(c * F + hf * H, H), H)

    def rs_copy(d, c, slot, src):
        return rcopy(src, rb.at[d, c, slot], rs_s.at[d, c, slot], rs_r.at[d, c, slot], z=zz(1 if d == 0 else -1))

    def first_hop(c):
        for d in range(2):
            for short in range(2):
                hf = d if short == 0 else 1 - d
                dist = 4 - short
                sb[d, c, short] = part[zz(dist if d == 0 else -dist), :, span(c, hf)].astype(bf16)
                rs_copy(d, c, 4 * short, sb.at[d, c, short]).start()

    def later_hop(c, hop):
        for d in range(2):
            for short in range(2):
                if short and hop == 4:
                    continue
                hf = d if short == 0 else 1 - d
                dist = 5 - hop - short
                slot = 4 * short + hop - 2
                rs_copy(d, c, slot, rb.at[d, c, slot]).wait_recv()
                mine = part[zz(dist if d == 0 else -dist), :, span(c, hf)]
                rb[d, c, slot] = (rb[d, c, slot].astype(f32) + mine).astype(bf16)
                rs_copy(d, c, slot + 1, rb.at[d, c, slot]).start()

    def finish(c):
        for d in range(2):
            rs_copy(d, c, 3, rb.at[d, c, 3]).wait_recv()
            rs_copy(d, c, 6, rb.at[d, c, 6]).wait_recv()
        total = inner[...]
        for hf in range(2):
            at = span(c, hf)
            got = part[z, :, at] + rb[hf, c, 3].astype(f32) + rb[1 - hf, c, 6].astype(f32)
            ng[:, at] = got
            t = got * gain[:, at] * tok[z, :, at].astype(f32)
            for q in range(H // 128):
                total = total + t[:, q * 128:(q + 1) * 128]
        inner[...] = total

    def gain_part(c):
        def one(t, carry):
            at = pl.ds(pl.multiple_of(c * F + t * 128, 128), 128)
            total = jnp.zeros((rows, 128), f32)
            for b in range(Z):
                total = total + part[b, :, at] * tok[b, :, at].astype(f32) * scl[b]
            gp[c, :, pl.ds(pl.multiple_of(t * 128, 128), 128)] = jnp.sum(total, axis=0, keepdims=True)
            return carry

        lax.fori_loop(0, F // 128, one, 0)

    def g_send(c):
        return rcopy(gp.at[c], gr.at[z], g_s.at[c], g_r.at[z], z=c)

    def gf_send(k):
        return rcopy(gf.at[z], gf.at[z], gf_s.at[k], gf_r.at[z], z=zz(k))

    gy_copy = rcopy(gs, gy, gy_s.at[0], gy_r.at[0], **direct)

    def forward_tile(t):
        n = jnp.where(yl == 0, t, 4 - t)
        cols = pl.ds(pl.multiple_of(n * 256, 256), 256)
        deep = dim // 4
        acc[...] = jnp.broadcast_to(bias[:, cols], acc.shape)

        def one(k, carry):
            at = pl.ds(pl.multiple_of(k * deep, deep), deep)
            lhs = nrm[:, :, at].reshape(Z * rows, deep)
            acc[...] += jnp.dot(lhs, w[at, cols], preferred_element_type=f32)
            return carry

        lax.fori_loop(0, 4, one, 0)

        def spin(b, carry):
            at = pl.ds(pl.multiple_of(b * rows, rows), rows)
            for h in range(2):
                x = acc[at, h * HEAD:(h + 1) * HEAD]
                r = x * cosv[yl, at, :] + pltpu.roll(x, HEAD // 2, 1) * sinv[yl, at, :]
                if h == 1:
                    r = jnp.where(n == 4, x, r)
                out[b, :, pl.ds(pl.multiple_of(n * 256 + h * HEAD, HEAD), HEAD)] = r.astype(bf16)
            return carry

        lax.fori_loop(0, Z, spin, 0)

    o_copy = rcopy(out.at[:, :, far], qkv_o.at[:, yl], o_s.at[0], o_r.at[0], **direct)
    o_local = pltpu.make_async_copy(out.at[:, :, own], qkv_o.at[:, yl], loc.at[8])

    inner[...] = jnp.zeros_like(inner)

    def iteration(i, carry):
        @pl.when(i < N)
        def _():
            backward_chunk(i)
            first_hop(i)

        for hop in (2, 3, 4):
            @pl.when((i >= hop - 1) & (i < N + hop - 1))
            def _(hop=hop):
                later_hop(i - hop + 1, hop)

        @pl.when(i >= 4)
        def _():
            finish(i - 4)

        @pl.when(i < N)
        def _():
            gain_part(i)

            @pl.when(i != z)
            def _():
                g_send(i).start()

        @pl.when(i == z + 1)
        def _():
            total = gp[z]
            for k in range(1, Z):
                spot = gr.at[zz(k)]
                rcopy(spot, spot, g_s.at[zz(k)], g_r.at[zz(k)], z=z).wait_recv()
                total = total + gr[zz(k)]
            gs[...] = total
            gy_copy.start()

        @pl.when(i == z + 2)
        def _():
            gy_copy.wait_recv()
            gf[z] = gs[...] + gy[...]
            for k in range(1, Z):
                gf_send(k).start()

        @pl.when(i < 3)
        def _():
            hand_on(i + 3)

        @pl.when((i == 4) | (i == 5))
        def _():
            hand_on(i + 2)

        @pl.when((i < 2) | ((i >= 5) & (i < 8)))
        def _():
            @pl.when(i == 5)
            def _():
                d_got(6).wait_recv()
                d_got(7).wait_recv()
            forward_tile(jnp.where(i < 2, i, i - 3))

        @pl.when(i == 7)
        def _():
            o_copy.start()
            o_local.start()
        return carry

    lax.fori_loop(0, N + 4, iteration, 0)

    mean = jnp.sum(inner[...], axis=1, keepdims=True) / dim
    s = scl[z]
    k3 = s * s * s * jnp.broadcast_to(mean, s.shape)
    s4 = jnp.concatenate([s] * 4, axis=1)
    k4 = jnp.concatenate([k3] * 4, axis=1)

    def last(i, carry):
        at = pl.ds(pl.multiple_of(i * 512, 512), 512)
        ng[:, at] = s4 * gain[:, at] * ng[:, at] - tok[z, :, at].astype(f32) * k4
        return carry

    outs = []
    for q in range(4):
        per = dim // 2048
        lax.fori_loop(q * per, (q + 1) * per, last, 0)
        at = pl.ds(q * (dim // 4), dim // 4)
        copy = pltpu.make_async_copy(ng.at[:, at], tg_o.at[:, at], loc.at[9 + q])
        copy.start()
        outs.append(copy)

    for k in range(1, Z):
        spot = gf.at[zz(k)]
        rcopy(spot, spot, gf_s.at[k], gf_r.at[zz(k)], z=z).wait_recv()
    g_out = pltpu.make_async_copy(gf, gg_o, loc.at[13])
    g_out.start()

    for d in range(2):
        for k in range(PER):
            ag_copy(d, k).wait_send()
    q_copy.wait_send()
    b_copy.wait_send()
    gy_copy.wait_send()

    def sent(c, carry):
        w_copy(c, 0).wait_send()
        w_copy(c, 1).wait_send()
        d_copy(c).wait_send()
        for d in range(2):
            for slot in range(PER):
                rs_copy(d, c, slot, rb.at[d, c, slot]).wait_send()

        @pl.when(c != z)
        def _():
            g_send(c).wait_send()
        return carry

    lax.fori_loop(0, N, sent, 0)
    for k in range(1, Z):
        gf_send(k).wait_send()
    o_copy.wait()
    o_local.wait()
    bg_copy.wait()
    g_out.wait()
    for copy in outs:
        copy.wait()


def tables(tokens_per):
    mp = 2 * Z
    block = np.arange(mp).reshape(Z, 2).T.reshape(-1)
    position = (block[:, None] * (SEQ_LEN // mp) + np.arange(tokens_per)[None, :]).reshape(-1)
    half = HEAD // 2
    inverse = np.exp(-np.log(1000000.0) * (2.0 * np.arange(half) / HEAD))
    angle = position[:, None].astype(np.float64) * inverse[None, :]
    c, s = np.cos(angle), np.sin(angle)
    shape = (2, Z * tokens_per, HEAD)
    return (
        np.concatenate([c, c], axis=1).astype(np.float32).reshape(shape),
        np.concatenate([-s, s], axis=1).astype(np.float32).reshape(shape),
    )


def shards(tokens, norm_gain, qkv_weight, qkv_bias, qkv_grad):
    rows, dim = tokens.shape
    width = qkv_weight.shape[1]
    F = dim // N
    H = F // 2
    both = 2 * width
    cos, sin = tables(rows)
    any_spec = pl.BlockSpec(memory_space=pl.ANY)
    dma = pltpu.SemaphoreType.DMA
    V = pltpu.VMEM
    qkv, tokens_grad, gain_grad, bias_grad = pl.pallas_call(
        kernel,
        name="qkv_ring",
        out_shape=(
            jax.ShapeDtypeStruct((Z, 2, rows, width), bf16),
            jax.ShapeDtypeStruct((rows, dim), f32),
            jax.ShapeDtypeStruct((Z, 1, F), f32),
            jax.ShapeDtypeStruct((1, width), f32),
        ),
        in_specs=[any_spec] * 7,
        out_specs=(any_spec,) * 4,
        scratch_shapes=[
            V((dim, both), bf16),
            V((Z, rows, dim), bf16),
            V((Z, rows, dim), bf16),
            V((Z, rows, dim), f32),
            V((2, N, PER, rows, H), bf16),
            V((2, N, 2, rows, H), bf16),
            V((Z, 2, rows, width), bf16),
            V((Z, rows, width), bf16),
            V((Z * rows, both), bf16),
            V((Z, rows, both), bf16),
            V((rows, dim), f32),
            V((Z, rows, 128), f32),
            V((rows, 128), f32),
            V((Z * rows, 256), f32),
            V((N, 1, F), f32),
            V((Z, 1, F), f32),
            V((1, F), f32),
            V((1, F), f32),
            V((Z, 1, F), f32),
            V((1, dim), f32),
            V((1, both), f32),
            V((1, width), f32),
            V(cos.shape, f32),
            V(sin.shape, f32),
            dma((2, PER)), dma((2, PER)),
            dma((2, N)), dma((2, N)),
            dma((N,)), dma((N,)),
            dma((2, N, PER)), dma((2, N, PER)),
            dma((1,)), dma((1,)),
            dma((1,)), dma((1,)),
            dma((1,)), dma((1,)),
            dma((Z,)), dma((Z,)),
            dma((1,)), dma((1,)),
            dma((Z,)), dma((Z,)),
            dma((14,)),
        ],
        compiler_params=pltpu.CompilerParams(
            collective_id=0, has_side_effects=True, vmem_limit_bytes=66_000_000
        ),
    )(
        tokens,
        qkv_weight,
        qkv_grad.reshape(Z, 2, rows, width),
        norm_gain.reshape(1, dim),
        qkv_bias.reshape(1, width),
        jnp.asarray(cos),
        jnp.asarray(sin),
    )
    return (
        qkv.reshape(2 * Z * rows, width),
        tokens_grad,
        gain_grad.reshape(dim),
        bias_grad.reshape(width),
    )


def solution(mesh):
    dp, mp = AXES[:3], AXES[3:]
    split = Mesh(mesh.devices.reshape(2, mesh.shape["dp"] // 4, 2, Z, 2), AXES)
    return jax.shard_map(
        shards,
        mesh=split,
        in_specs=(P(AXES, None), P(), P(None, mp), P(mp), P(dp, mp)),
        out_specs=(P(dp, mp), P(AXES, None), P(dp), P(AXES)),
        check_vma=False,
    )
```

```python
import functools

import jax
import jax.numpy as jnp
import numpy as np
from jax import lax
from jax.experimental import pallas as pl
from jax.experimental.pallas import tpu as pltpu
from jax.sharding import Mesh
from jax.sharding import PartitionSpec as P

HEAD = 128
SEQ_LEN = 32768
MESH = pl.DeviceIdType.MESH
AXES = ("yh", "x", "core", "z", "yl")
Z = 8
N = 8
PER = 7
f32 = jnp.float32
bf16 = jnp.bfloat16


def rcopy(src, dst, ssem, rsem, **where):
    return pltpu.make_async_remote_copy(
        src_ref=src, dst_ref=dst, send_sem=ssem, recv_sem=rsem, device_id=where, device_id_type=MESH
    )


def kernel(
    tok_h, w_h, qg_h, gain_h, bias_h, cos_h, sin_h,
    qkv_o, tg_o, gg_o, bg_o,
    w, tok, nrm, part, rb, sb, qb, qp, jl, out, ng, scl, inner, acc,
    gp, gr, gs, gy, gf, gain, bias, b_own, b_far, bgv, bg1, cosv, sinv,
    ag_r, ag_s, w_r, w_s, x_r, x_s, d_r, d_s, rs_r, rs_s, q_r, q_s, b_r, b_s, o_r, o_s,
    g_r, g_s, gy_r, gy_s, gf_r, gf_s, loc,
):
    rows, dim = tok_h.shape
    width = w_h.shape[1]
    F = dim // N
    H = F // 2
    half = dim // 2
    yh, x, core, z, yl = (lax.axis_index(a) for a in AXES)

    def zz(k):
        return lax.rem(z + (k + Z), Z)

    direct = {"yl": 1 - yl}
    other = {"yh": 1 - yh, "yl": 1 - yl}
    sibling = {"core": 1 - core}
    nx = lax.axis_size("x")
    beside = [{"x": lax.rem(x + 1, nx)}, {"x": lax.rem(x + nx - 1, nx)}]
    side = lax.rem(x, 2)
    own = pl.ds(pl.multiple_of(yl * width, 128), width)
    far = pl.ds(pl.multiple_of((1 - yl) * width, 128), width)

    local = [
        pltpu.make_async_copy(tok_h, tok.at[z], loc.at[0]),
        pltpu.make_async_copy(qg_h, qb, loc.at[1]),
        pltpu.make_async_copy(cos_h, cosv, loc.at[2]),
        pltpu.make_async_copy(sin_h, sinv, loc.at[3]),
        pltpu.make_async_copy(gain_h, gain, loc.at[4]),
        pltpu.make_async_copy(bias_h, b_own, loc.at[5]),
        pltpu.make_async_copy(w_h, w.at[:, own], loc.at[6]),
    ]
    for copy in local:
        copy.start()

    barrier = pltpu.get_barrier_semaphore()
    for k in range(1, Z):
        pl.semaphore_signal(barrier, inc=1, device_id={"z": zz(k)}, device_id_type=MESH)
    for where in (direct, other, sibling, *beside):
        pl.semaphore_signal(barrier, inc=1, device_id=where, device_id_type=MESH)
    pl.semaphore_wait(barrier, Z + 4)

    def ag_half(d, k):
        return d if k % 2 == 0 else 1 - d

    def ag_copy(d, k):
        step = k // 2
        block = zz(-step) if d == 0 else zz(step)
        cols = pl.ds(ag_half(d, k) * half, half)
        src = tok_h.at[:, cols] if step == 0 else tok.at[block, :, cols]
        return rcopy(src, tok.at[block, :, cols], ag_s.at[d, k], ag_r.at[d, k], z=zz(1 if d == 0 else -1))

    for k in range(2):
        for d in range(2):
            ag_copy(d, k).start()

    q_copy = rcopy(qg_h.at[:, 1 - yl], qp, q_s.at[0], q_r.at[0], **direct)
    q_copy.start()
    b_copy = rcopy(bias_h, b_far, b_s.at[0], b_r.at[0], **direct)
    b_copy.start()

    piece = F // 8

    def w_rows(j, par, who, s, n):
        return pl.ds(pl.multiple_of(j * F + par * 4 * piece + who * 2 * piece + s * piece, piece), n * piece)

    def w_copy(j, s):
        at = w_rows(j, side, core, s, 1)
        return rcopy(w_h.at[at], w.at[at, own], w_s.at[s, j], w_r.at[s, j], **(direct if s == 0 else other))

    def w_got(j, s):
        spot = w.at[w_rows(j, side, core, s, 1), far]
        return rcopy(spot, spot, w_s.at[s, j], w_r.at[s, j], **(direct if s == 0 else other))

    def x_copy(j, s):
        spot = w.at[w_rows(j, side, core, s, 1), far]
        return rcopy(spot, spot, x_s.at[s, j], x_r.at[s, j], **beside[s])

    def x_got(j, s):
        spot = w.at[w_rows(j, 1 - side, core, s, 1), far]
        return rcopy(spot, spot, x_s.at[s, j], x_r.at[s, j], **beside[1 - s])

    def d_copy(j, k):
        spot = w.at[w_rows(j, side if k == 0 else 1 - side, core, 0, 2), far]
        return rcopy(spot, spot, d_s.at[k, j], d_r.at[k, j], **sibling)

    def d_got(j, k):
        spot = w.at[w_rows(j, side if k == 0 else 1 - side, 1 - core, 0, 2), far]
        return rcopy(spot, spot, d_s.at[k, j], d_r.at[k, j], **sibling)

    def hand_on(j):
        for s in range(2):
            w_got(j, s).wait_recv()
            x_copy(j, s).start()
        d_copy(j, 0).start()

    def hand_over(j):
        for s in range(2):
            x_got(j, s).wait_recv()
        d_copy(j, 1).start()

    for j in range(N):
        w_copy(j, 0).start()
        w_copy(j, 1).start()

    def norm_block(b):
        step = min(512, dim)

        def sq(i, total):
            v = tok[b, :, pl.ds(pl.multiple_of(i * step, step), step)].astype(f32)
            v = v * v
            for q in range(step // 128):
                total = total + v[:, q * 128:(q + 1) * 128]
            return total

        total = lax.fori_loop(0, dim // step, sq, jnp.zeros((rows, 128), f32))
        mean = jnp.sum(total, axis=1, keepdims=True) / dim
        s = jnp.broadcast_to(lax.rsqrt(mean + 1e-06), (rows, 128))
        scl[b] = s
        wide = jnp.concatenate([s] * (step // 128), axis=1)

        def put(i, carry):
            at = pl.ds(pl.multiple_of(i * step, step), step)
            v = tok[b, :, at].astype(f32)
            nrm[b, :, at] = (v * wide * gain[:, at]).astype(bf16)
            return carry

        lax.fori_loop(0, dim // step, put, 0)

    def turn_back(x, line, b, is_value):
        c = cosv[line, pl.ds(pl.multiple_of(b * rows, rows), rows), :]
        s = sinv[line, pl.ds(pl.multiple_of(b * rows, rows), rows), :]
        r = x * c - pltpu.roll(x, HEAD // 2, 1) * s
        return r if is_value is None else jnp.where(is_value, x, r)

    heads = width // HEAD

    def own_columns():
        bgv[...] = jnp.zeros_like(bgv)

        def one(b, carry):
            at = pl.ds(pl.multiple_of(b * rows, rows), rows)
            for h in range(heads):
                value = (yl == 1) if h == heads - 1 else None
                hs = pl.ds(h * HEAD, HEAD)
                for line in range(2):
                    r = turn_back(qb[b, line, :, hs].astype(f32), line, b, value)
                    bgv[:, hs] += jnp.sum(r, axis=0, keepdims=True)
                r = turn_back(qb[b, yl, :, hs].astype(f32), yl, b, value)
                jl[at, pl.ds(pl.multiple_of(yl * width + h * HEAD, HEAD), HEAD)] = r.astype(bf16)
            return carry

        lax.fori_loop(0, Z, one, 0)

    def far_columns():
        def one(b, carry):
            at = pl.ds(pl.multiple_of(b * rows, rows), rows)
            for h in range(heads):
                value = (yl == 0) if h == heads - 1 else None
                r = turn_back(qp[b, :, pl.ds(h * HEAD, HEAD)].astype(f32), yl, b, value)
                jl[at, pl.ds(pl.multiple_of((1 - yl) * width + h * HEAD, HEAD), HEAD)] = r.astype(bf16)
            return carry

        lax.fori_loop(0, Z, one, 0)

    bt = min(256, F)

    def backward_part(c, first, count):
        def one(t, carry):
            at = pl.ds(pl.multiple_of(c * F + t * bt, bt), bt)
            got = lax.dot_general(jl[...], w[at, :], (((1,), (1,)), ((), ())), preferred_element_type=f32)
            part[:, :, at] = got.reshape(Z, rows, bt)
            return carry

        lax.fori_loop(first, first + count, one, 0)

    def weights_here(c):
        d_got(c, 0).wait_recv()
        d_got(c, 1).wait_recv()

    def backward_chunk(c):
        weights_here(c)
        backward_part(c, 0, F // bt)

    def span(c, hf):
        return pl.ds(pl.multiple_of(c * F + hf * H, H), H)

    def rs_copy(d, c, slot, src):
        return rcopy(src, rb.at[d, c, slot], rs_s.at[d, c, slot], rs_r.at[d, c, slot], z=zz(1 if d == 0 else -1))

    def first_hop(c):
        for d in range(2):
            for short in range(2):
                hf = d if short == 0 else 1 - d
                dist = 4 - short
                sb[d, c, short] = part[zz(dist if d == 0 else -dist), :, span(c, hf)].astype(bf16)
                rs_copy(d, c, 4 * short, sb.at[d, c, short]).start()

    def later_hop(c, hop):
        def one(d, short):
            hf = d if short == 0 else 1 - d
            dist = 4 - hop - short
            slot = 4 * short + hop - 1
            rs_copy(d, c, slot, rb.at[d, c, slot]).wait_recv()
            mine = part[zz(dist if d == 0 else -dist), :, span(c, hf)]
            rb[d, c, slot] = (rb[d, c, slot].astype(f32) + mine).astype(bf16)
            rs_copy(d, c, slot + 1, rb.at[d, c, slot]).start()

        one(0, 0)
        one(1, 0)

        @pl.when(hop < 3)
        def _():
            one(0, 1)
            one(1, 1)

    def finish(c):
        for d in range(2):
            rs_copy(d, c, 3, rb.at[d, c, 3]).wait_recv()
            rs_copy(d, c, 6, rb.at[d, c, 6]).wait_recv()
        total = inner[...]
        for hf in range(2):
            at = span(c, hf)
            got = part[z, :, at] + rb[hf, c, 3].astype(f32) + rb[1 - hf, c, 6].astype(f32)
            ng[:, at] = got
            t = got * gain[:, at] * tok[z, :, at].astype(f32)
            for q in range(H // 128):
                total = total + t[:, q * 128:(q + 1) * 128]
        inner[...] = total

    def gain_part(c):
        def one(t, carry):
            at = pl.ds(pl.multiple_of(c * F + t * 128, 128), 128)
            total = jnp.zeros((rows, 128), f32)
            for b in range(Z):
                total = total + part[b, :, at] * tok[b, :, at].astype(f32) * scl[b]
            gp[c, :, pl.ds(pl.multiple_of(t * 128, 128), 128)] = jnp.sum(total, axis=0, keepdims=True)
            return carry

        lax.fori_loop(0, F // 128, one, 0)

    def g_send(c):
        return rcopy(gp.at[c], gr.at[z], g_s.at[c], g_r.at[z], z=c)

    def gf_send(k):
        return rcopy(gf.at[z], gf.at[z], gf_s.at[k], gf_r.at[z], z=zz(k))

    gy_copy = rcopy(gs, gy, gy_s.at[0], gy_r.at[0], **direct)

    def forward_quarter(t, k):
        n = jnp.where(yl == 0, 4 - t, t)
        cols = pl.ds(pl.multiple_of(n * 256, 256), 256)
        deep = dim // 4

        @pl.when(k == 0)
        def _():
            acc[...] = jnp.broadcast_to(bias[:, cols], acc.shape)

        at = pl.ds(pl.multiple_of(k * deep, deep), deep)
        lhs = nrm[:, :, at].reshape(Z * rows, deep)
        acc[...] += jnp.dot(lhs, w[at, cols], preferred_element_type=f32)

        def spin(b, carry):
            at = pl.ds(pl.multiple_of(b * rows, rows), rows)
            for h in range(2):
                x = acc[at, h * HEAD:(h + 1) * HEAD]
                r = x * cosv[yl, at, :] + pltpu.roll(x, HEAD // 2, 1) * sinv[yl, at, :]
                if h == 1:
                    r = jnp.where(n == 4, x, r)
                out[b, :, pl.ds(pl.multiple_of(n * 256 + h * HEAD, HEAD), HEAD)] = r.astype(bf16)
            return carry

        @pl.when(k == 3)
        def _():
            lax.fori_loop(0, Z, spin, 0)

    o_copy = rcopy(out.at[:, :, far], qkv_o.at[:, yl], o_s.at[0], o_r.at[0], **direct)
    o_local = pltpu.make_async_copy(out.at[:, :, own], qkv_o.at[:, yl], loc.at[8])

    inner[...] = jnp.zeros_like(inner)

    for k in range(1, 5):
        local[k].wait()
    own_columns()
    local[0].wait()
    norm_block(z)
    local[5].wait()
    bg1[...] = bgv[...].reshape(width)
    bg_copy = pltpu.make_async_copy(bg1, bg_o, loc.at[7])
    bg_copy.start()

    for k in range(PER):
        for d in range(2):
            block = zz(-1 - k // 2) if d == 0 else zz(1 + k // 2)
            cols = pl.ds(ag_half(d, k) * half, half)
            spot = tok.at[block, :, cols]
            rcopy(spot, spot, ag_s.at[d, k], ag_r.at[d, k], z=zz(1)).wait_recv()
            if k + 2 < PER:
                ag_copy(d, k + 2).start()
        for j in {1: (0,), 2: (1, 2), 3: (3, 4), 4: (5,), 5: (6, 7)}.get(k, ()):
            hand_on(j)
        for j in {3: (0,), 4: (1, 2), 5: (3, 4), 6: (5,)}.get(k, ()):
            hand_over(j)
        if k == 1:
            q_copy.wait_recv()
            b_copy.wait_recv()
            bias[:, own] = b_own[...].reshape(1, width)
            bias[:, far] = b_far[...].reshape(1, width)
            far_columns()
        if k in (1, 3):
            norm_block(zz(-1 - k // 2))
            norm_block(zz(1 + k // 2))
        if k == 4:
            local[6].wait()
            backward_chunk(0)
        if k == 5:
            first_hop(0)
            backward_chunk(1)
            first_hop(1)
            norm_block(zz(-3))
            norm_block(zz(3))
            backward_chunk(2)
            first_hop(2)
        if k == 6:
            backward_chunk(3)
            first_hop(3)
            norm_block(zz(4))

    def event(e, carry):
        r = lax.rem(e, 16)
        hop = r // 4
        c = e // 16 * 4 + lax.rem(r, 4)

        @pl.when((hop == 0) & (e < 32))
        def _():
            first_hop(c)

        @pl.when((hop > 0) & (e < 32))
        def _():
            later_hop(c, hop)

        @pl.when((e == 4) | (e == 6))
        def _():
            hand_over(6 + (e - 4) // 2)

        @pl.when(e < 12)
        def _():
            c = 4 + (e - 4) // 2
            odd = lax.rem(e, 2)

            @pl.when(odd == 0)
            def _():
                weights_here(c)
            backward_part(c, odd * (F // bt // 2), F // bt // 2)

        @pl.when((e < 8) | ((e >= 12) & (e < 16)))
        def _():
            c = jnp.where(e < 8, e - 4, e - 8)
            gain_part(c)

            @pl.when(c != z)
            def _():
                g_send(c).start()

        @pl.when((e >= 12) & (e < 32))
        def _():
            forward_quarter((e - 12) // 4, lax.rem(e, 4))

        @pl.when(e == 21)
        def _():
            total = gp[z]
            for k in range(1, Z):
                spot = gr.at[zz(k)]
                rcopy(spot, spot, g_s.at[zz(k)], g_r.at[zz(k)], z=zz(1)).wait_recv()
                total = total + gr[zz(k)]
            gs[...] = total
            gy_copy.start()

        @pl.when(e == 24)
        def _():
            o_copy.start()

        @pl.when(e == 25)
        def _():
            gy_copy.wait_recv()
            gf[z] = gs[...] + gy[...]
            for k in range(1, Z):
                gf_send(k).start()

        @pl.when(((e >= 24) & (e < 28)) | (e >= 32))
        def _():
            finish(jnp.where(e < 28, e - 24, e - 28))
        return carry

    lax.fori_loop(4, 36, event, 0)
    o_local.start()

    mean = jnp.sum(inner[...], axis=1, keepdims=True) / dim
    s = scl[z]
    k3 = s * s * s * jnp.broadcast_to(mean, s.shape)
    s4 = jnp.concatenate([s] * 4, axis=1)
    k4 = jnp.concatenate([k3] * 4, axis=1)

    def last(i, carry):
        at = pl.ds(pl.multiple_of(i * 512, 512), 512)
        ng[:, at] = s4 * gain[:, at] * ng[:, at] - tok[z, :, at].astype(f32) * k4
        return carry

    outs = []
    for q in range(4):
        per = dim // 2048
        lax.fori_loop(q * per, (q + 1) * per, last, 0)
        at = pl.ds(q * (dim // 4), dim // 4)
        copy = pltpu.make_async_copy(ng.at[:, at], tg_o.at[:, at], loc.at[9 + q])
        copy.start()
        outs.append(copy)

    for k in range(1, Z):
        spot = gf.at[zz(k)]
        rcopy(spot, spot, gf_s.at[k], gf_r.at[zz(k)], z=zz(1)).wait_recv()
    g_out = pltpu.make_async_copy(gf, gg_o, loc.at[13])
    g_out.start()

    for d in range(2):
        for k in range(PER):
            ag_copy(d, k).wait_send()
    q_copy.wait_send()
    b_copy.wait_send()
    gy_copy.wait_send()

    def sent(c, carry):
        w_copy(c, 0).wait_send()
        w_copy(c, 1).wait_send()
        for k in range(2):
            x_copy(c, k).wait_send()
            d_copy(c, k).wait_send()
        for d in range(2):
            for slot in range(PER):
                rs_copy(d, c, slot, rb.at[d, c, slot]).wait_send()

        @pl.when(c != z)
        def _():
            g_send(c).wait_send()
        return carry

    lax.fori_loop(0, N, sent, 0)
    for k in range(1, Z):
        gf_send(k).wait_send()
    o_copy.wait()
    o_local.wait()
    bg_copy.wait()
    g_out.wait()
    for copy in outs:
        copy.wait()


def tables(tokens_per):
    mp = 2 * Z
    block = np.arange(mp).reshape(Z, 2).T.reshape(-1)
    position = (block[:, None] * (SEQ_LEN // mp) + np.arange(tokens_per)[None, :]).reshape(-1)
    half = HEAD // 2
    inverse = np.exp(-np.log(1000000.0) * (2.0 * np.arange(half) / HEAD))
    angle = position[:, None].astype(np.float64) * inverse[None, :]
    c, s = np.cos(angle), np.sin(angle)
    shape = (2, Z * tokens_per, HEAD)
    return (
        np.concatenate([c, c], axis=1).astype(np.float32).reshape(shape),
        np.concatenate([-s, s], axis=1).astype(np.float32).reshape(shape),
    )


def shards(tokens, norm_gain, qkv_weight, qkv_bias, qkv_grad):
    rows, dim = tokens.shape
    width = qkv_weight.shape[1]
    F = dim // N
    H = F // 2
    both = 2 * width
    cos, sin = tables(rows)
    any_spec = pl.BlockSpec(memory_space=pl.ANY)
    dma = pltpu.SemaphoreType.DMA
    V = pltpu.VMEM
    qkv, tokens_grad, gain_grad, bias_grad = pl.pallas_call(
        kernel,
        name="qkv_ring",
        out_shape=(
            jax.ShapeDtypeStruct((Z, 2, rows, width), bf16),
            jax.ShapeDtypeStruct((rows, dim), f32),
            jax.ShapeDtypeStruct((Z, 1, F), f32),
            jax.ShapeDtypeStruct((width,), f32),
        ),
        in_specs=[any_spec] * 7,
        out_specs=(any_spec,) * 4,
        scratch_shapes=[
            V((dim, both), bf16),
            V((Z, rows, dim), bf16),
            V((Z, rows, dim), bf16),
            V((Z, rows, dim), f32),
            V((2, N, PER, rows, H), bf16),
            V((2, N, 2, rows, H), bf16),
            V((Z, 2, rows, width), bf16),
            V((Z, rows, width), bf16),
            V((Z * rows, both), bf16),
            V((Z, rows, both), bf16),
            V((rows, dim), f32),
            V((Z, rows, 128), f32),
            V((rows, 128), f32),
            V((Z * rows, 256), f32),
            V((N, 1, F), f32),
            V((Z, 1, F), f32),
            V((1, F), f32),
            V((1, F), f32),
            V((Z, 1, F), f32),
            V((1, dim), f32),
            V((1, both), f32),
            V((width,), f32),
            V((width,), f32),
            V((1, width), f32),
            V((width,), f32),
            V(cos.shape, f32),
            V(sin.shape, f32),
            dma((2, PER)), dma((2, PER)),
            dma((2, N)), dma((2, N)),
            dma((2, N)), dma((2, N)),
            dma((2, N)), dma((2, N)),
            dma((2, N, PER)), dma((2, N, PER)),
            dma((1,)), dma((1,)),
            dma((1,)), dma((1,)),
            dma((1,)), dma((1,)),
            dma((Z,)), dma((Z,)),
            dma((1,)), dma((1,)),
            dma((Z,)), dma((Z,)),
            dma((14,)),
        ],
        compiler_params=pltpu.CompilerParams(
            collective_id=0, has_side_effects=True, vmem_limit_bytes=66_000_000
        ),
    )(
        tokens,
        qkv_weight,
        qkv_grad.reshape(Z, 2, rows, width),
        norm_gain.reshape(1, dim),
        qkv_bias,
        jnp.asarray(cos),
        jnp.asarray(sin),
    )
    return (
        qkv.reshape(2 * Z * rows, width),
        tokens_grad,
        gain_grad.reshape(dim),
        bias_grad,
    )


def solution(mesh):
    dp, mp = AXES[:3], AXES[3:]
    split = Mesh(mesh.devices.reshape(2, mesh.shape["dp"] // 4, 2, Z, 2), AXES)
    return jax.shard_map(
        shards,
        mesh=split,
        in_specs=(P(AXES, None), P(), P(None, mp), P(mp), P(dp, mp)),
        out_specs=(P(dp, mp), P(AXES, None), P(dp), P(AXES)),
        check_vma=False,
    )
```

```python
import functools

import jax
import jax.numpy as jnp
import numpy as np
from jax import lax
from jax.experimental import pallas as pl
from jax.experimental.pallas import tpu as pltpu
from jax.sharding import Mesh
from jax.sharding import PartitionSpec as P

HEAD = 128
SEQ_LEN = 32768
MESH = pl.DeviceIdType.MESH
AXES = ("yh", "x", "core", "z", "yl")
Z = 8
N = 8
PER = 7
f32 = jnp.float32
bf16 = jnp.bfloat16


def rcopy(src, dst, ssem, rsem, **where):
    return pltpu.make_async_remote_copy(
        src_ref=src, dst_ref=dst, send_sem=ssem, recv_sem=rsem, device_id=where, device_id_type=MESH
    )


def kernel(
    tok_h, w_h, qg_h, gain_h, bias_h, cos_h, sin_h,
    qkv_o, ng_o, st_o, gg_o, bg_o,
    w, tok, nrm, part, rb, sb, qb, qp, jl, out, ng, st, scl, inner, acc,
    gp, gr, gs, gy, gf, gain, bias, b_own, b_far, bgv, bg1, cosv, sinv,
    ag_r, ag_s, w_r, w_s, x_r, x_s, d_r, d_s, rs_r, rs_s, q_r, q_s, b_r, b_s, o_r, o_s,
    g_r, g_s, gy_r, gy_s, gf_r, gf_s, ng_s, loc,
):
    rows, dim = tok_h.shape
    width = w_h.shape[1]
    F = dim // N
    H = F // 2
    half = dim // 2
    yh, x, core, z, yl = (lax.axis_index(a) for a in AXES)

    def zz(k):
        return lax.rem(z + (k + Z), Z)

    direct = {"yl": 1 - yl}
    other = {"yh": 1 - yh, "yl": 1 - yl}
    sibling = {"core": 1 - core}
    nx = lax.axis_size("x")
    beside = [{"x": lax.rem(x + 1, nx)}, {"x": lax.rem(x + nx - 1, nx)}]
    side = lax.rem(x, 2)
    own = pl.ds(pl.multiple_of(yl * width, 128), width)
    far = pl.ds(pl.multiple_of((1 - yl) * width, 128), width)

    local = [
        pltpu.make_async_copy(tok_h, tok.at[z], loc.at[0]),
        pltpu.make_async_copy(qg_h, qb, loc.at[1]),
        pltpu.make_async_copy(cos_h, cosv, loc.at[2]),
        pltpu.make_async_copy(sin_h, sinv, loc.at[3]),
        pltpu.make_async_copy(gain_h, gain, loc.at[4]),
        pltpu.make_async_copy(bias_h, b_own, loc.at[5]),
        pltpu.make_async_copy(w_h, w.at[:, own], loc.at[6]),
    ]
    for copy in local:
        copy.start()

    barrier = pltpu.get_barrier_semaphore()
    for where in ({"z": zz(1)}, {"z": zz(-1)}, direct, other, sibling, *beside):
        pl.semaphore_signal(barrier, inc=1, device_id=where, device_id_type=MESH)
    pl.semaphore_wait(barrier, 7)
    local[0].wait()

    def ag_half(d, k):
        return d if k % 2 == 0 else 1 - d

    def ag_copy(d, k):
        step = k // 2
        block = zz(-step) if d == 0 else zz(step)
        cols = pl.ds(ag_half(d, k) * half, half)
        spot = tok.at[block, :, cols]
        return rcopy(spot, spot, ag_s.at[d, k], ag_r.at[d, k], z=zz(1 if d == 0 else -1))

    for k in range(2):
        for d in range(2):
            ag_copy(d, k).start()

    q_copy = rcopy(qg_h.at[:, 1 - yl], qp, q_s.at[0], q_r.at[0], **direct)
    q_copy.start()
    b_copy = rcopy(bias_h, b_far, b_s.at[0], b_r.at[0], **direct)
    b_copy.start()

    piece = F // 8

    def w_rows(j, par, who, s, n):
        return pl.ds(pl.multiple_of(j * F + par * 4 * piece + who * 2 * piece + s * piece, piece), n * piece)

    def w_copy(j, s):
        at = w_rows(j, side, core, s, 1)
        return rcopy(w_h.at[at], w.at[at, own], w_s.at[s, j], w_r.at[s, j], **(direct if s == 0 else other))

    def w_got(j, s):
        spot = w.at[w_rows(j, side, core, s, 1), far]
        return rcopy(spot, spot, w_s.at[s, j], w_r.at[s, j], **(direct if s == 0 else other))

    def x_copy(j, s):
        spot = w.at[w_rows(j, side, core, s, 1), far]
        return rcopy(spot, spot, x_s.at[s, j], x_r.at[s, j], **beside[s])

    def x_got(j, s):
        spot = w.at[w_rows(j, 1 - side, core, s, 1), far]
        return rcopy(spot, spot, x_s.at[s, j], x_r.at[s, j], **beside[1 - s])

    def d_copy(j, k):
        spot = w.at[w_rows(j, side if k == 0 else 1 - side, core, 0, 2), far]
        return rcopy(spot, spot, d_s.at[k, j], d_r.at[k, j], **sibling)

    def d_got(j, k):
        spot = w.at[w_rows(j, side if k == 0 else 1 - side, 1 - core, 0, 2), far]
        return rcopy(spot, spot, d_s.at[k, j], d_r.at[k, j], **sibling)

    def hand_on(j):
        for s in range(2):
            w_got(j, s).wait_recv()
            x_copy(j, s).start()
        d_copy(j, 0).start()

    def hand_over(j):
        for s in range(2):
            x_got(j, s).wait_recv()
        d_copy(j, 1).start()

    for j in range(N):
        w_copy(j, 0).start()
        w_copy(j, 1).start()

    def norm_block(b):
        step = min(512, dim)

        def sq(i, total):
            v = tok[b, :, pl.ds(pl.multiple_of(i * step, step), step)].astype(f32)
            v = v * v
            for q in range(step // 128):
                total = total + v[:, q * 128:(q + 1) * 128]
            return total

        total = lax.fori_loop(0, dim // step, sq, jnp.zeros((rows, 128), f32))
        mean = jnp.sum(total, axis=1, keepdims=True) / dim
        s = jnp.broadcast_to(lax.rsqrt(mean + 1e-06), (rows, 128))
        scl[b] = s
        wide = jnp.concatenate([s] * (step // 128), axis=1)

        def put(i, carry):
            at = pl.ds(pl.multiple_of(i * step, step), step)
            v = tok[b, :, at].astype(f32)
            nrm[b, :, at] = (v * wide * gain[:, at]).astype(bf16)
            return carry

        lax.fori_loop(0, dim // step, put, 0)

    def turn_back(x, line, b, is_value):
        c = cosv[line, pl.ds(pl.multiple_of(b * rows, rows), rows), :]
        s = sinv[line, pl.ds(pl.multiple_of(b * rows, rows), rows), :]
        r = x * c - pltpu.roll(x, HEAD // 2, 1) * s
        return r if is_value is None else jnp.where(is_value, x, r)

    heads = width // HEAD

    def own_columns():
        bgv[...] = jnp.zeros_like(bgv)

        def one(b, carry):
            at = pl.ds(pl.multiple_of(b * rows, rows), rows)
            for h in range(heads):
                value = (yl == 1) if h == heads - 1 else None
                hs = pl.ds(h * HEAD, HEAD)
                for line in range(2):
                    r = turn_back(qb[b, line, :, hs].astype(f32), line, b, value)
                    bgv[:, hs] += jnp.sum(r, axis=0, keepdims=True)
                r = turn_back(qb[b, yl, :, hs].astype(f32), yl, b, value)
                jl[at, pl.ds(pl.multiple_of(yl * width + h * HEAD, HEAD), HEAD)] = r.astype(bf16)
            return carry

        lax.fori_loop(0, Z, one, 0)

    def far_columns():
        def one(b, carry):
            at = pl.ds(pl.multiple_of(b * rows, rows), rows)
            for h in range(heads):
                value = (yl == 0) if h == heads - 1 else None
                r = turn_back(qp[b, :, pl.ds(h * HEAD, HEAD)].astype(f32), yl, b, value)
                jl[at, pl.ds(pl.multiple_of((1 - yl) * width + h * HEAD, HEAD), HEAD)] = r.astype(bf16)
            return carry

        lax.fori_loop(0, Z, one, 0)

    bt = min(256, F)

    def backward_part(c, first, count):
        def one(t, carry):
            at = pl.ds(pl.multiple_of(c * F + t * bt, bt), bt)
            got = lax.dot_general(jl[...], w[at, :], (((1,), (1,)), ((), ())), preferred_element_type=f32)
            part[:, :, at] = got.reshape(Z, rows, bt)
            return carry

        lax.fori_loop(first, first + count, one, 0)

    def weights_here(c):
        d_got(c, 0).wait_recv()
        d_got(c, 1).wait_recv()

    def backward_chunk(c):
        weights_here(c)
        backward_part(c, 0, F // bt)

    def span(c, hf):
        return pl.ds(pl.multiple_of(c * F + hf * H, H), H)

    def rs_copy(d, c, slot, src):
        return rcopy(src, rb.at[d, c, slot], rs_s.at[d, c, slot], rs_r.at[d, c, slot], z=zz(1 if d == 0 else -1))

    def first_hop(c):
        for d in range(2):
            for short in range(2):
                hf = d if short == 0 else 1 - d
                dist = 4 - short
                sb[d, c, short] = part[zz(dist if d == 0 else -dist), :, span(c, hf)].astype(bf16)
                rs_copy(d, c, 4 * short, sb.at[d, c, short]).start()

    def later_hop(c, hop):
        def one(d, short):
            hf = d if short == 0 else 1 - d
            dist = 4 - hop - short
            slot = 4 * short + hop - 1
            rs_copy(d, c, slot, rb.at[d, c, slot]).wait_recv()
            mine = part[zz(dist if d == 0 else -dist), :, span(c, hf)]
            rb[d, c, slot] = (rb[d, c, slot].astype(f32) + mine).astype(bf16)
            rs_copy(d, c, slot + 1, rb.at[d, c, slot]).start()

        one(0, 0)
        one(1, 0)

        @pl.when(hop < 3)
        def _():
            one(0, 1)
            one(1, 1)

    def ng_copy(c):
        at = pl.ds(pl.multiple_of(c * F, F), F)
        return pltpu.make_async_copy(ng.at[:, at], ng_o.at[:, at], ng_s.at[c])

    def finish(c):
        for d in range(2):
            rs_copy(d, c, 3, rb.at[d, c, 3]).wait_recv()
            rs_copy(d, c, 6, rb.at[d, c, 6]).wait_recv()
        total = inner[...]
        for hf in range(2):
            at = span(c, hf)
            got = part[z, :, at] + rb[hf, c, 3].astype(f32) + rb[1 - hf, c, 6].astype(f32)
            ng[:, at] = got
            t = got * gain[:, at] * tok[z, :, at].astype(f32)
            for q in range(H // 128):
                total = total + t[:, q * 128:(q + 1) * 128]
        inner[...] = total
        ng_copy(c).start()

    def gain_part(c):
        def one(t, carry):
            at = pl.ds(pl.multiple_of(c * F + t * 128, 128), 128)
            total = jnp.zeros((rows, 128), f32)
            for b in range(Z):
                total = total + part[b, :, at] * tok[b, :, at].astype(f32) * scl[b]
            gp[c, :, pl.ds(pl.multiple_of(t * 128, 128), 128)] = jnp.sum(total, axis=0, keepdims=True)
            return carry

        lax.fori_loop(0, F // 128, one, 0)

    def g_send(c):
        return rcopy(gp.at[c], gr.at[z], g_s.at[c], g_r.at[z], z=c)

    def gf_send(k):
        return rcopy(gf.at[z], gf.at[z], gf_s.at[k], gf_r.at[z], z=zz(k))

    gy_copy = rcopy(gs, gy, gy_s.at[0], gy_r.at[0], **direct)

    def forward_quarter(t, k):
        n = jnp.where(yl == 0, 4 - t, t)
        cols = pl.ds(pl.multiple_of(n * 256, 256), 256)
        deep = dim // 4

        @pl.when(k == 0)
        def _():
            acc[...] = jnp.broadcast_to(bias[:, cols], acc.shape)

        at = pl.ds(pl.multiple_of(k * deep, deep), deep)
        lhs = nrm[:, :, at].reshape(Z * rows, deep)
        acc[...] += jnp.dot(lhs, w[at, cols], preferred_element_type=f32)

        def spin(b, carry):
            at = pl.ds(pl.multiple_of(b * rows, rows), rows)
            for h in range(2):
                x = acc[at, h * HEAD:(h + 1) * HEAD]
                r = x * cosv[yl, at, :] + pltpu.roll(x, HEAD // 2, 1) * sinv[yl, at, :]
                if h == 1:
                    r = jnp.where(n == 4, x, r)
                out[b, :, pl.ds(pl.multiple_of(n * 256 + h * HEAD, HEAD), HEAD)] = r.astype(bf16)
            return carry

        @pl.when(k == 3)
        def _():
            lax.fori_loop(0, Z, spin, 0)

    o_copy = rcopy(out.at[:, :, far], qkv_o.at[:, yl], o_s.at[0], o_r.at[0], **direct)
    o_local = pltpu.make_async_copy(out.at[:, :, own], qkv_o.at[:, yl], loc.at[8])

    g_out = pltpu.make_async_copy(gf, gg_o, loc.at[10])
    inner[...] = jnp.zeros_like(inner)

    for k in range(1, 5):
        local[k].wait()
    own_columns()
    norm_block(z)
    local[5].wait()
    bg1[...] = bgv[...].reshape(width)
    bg_copy = pltpu.make_async_copy(bg1, bg_o, loc.at[7])
    bg_copy.start()

    for k in range(PER):
        for d in range(2):
            block = zz(-1 - k // 2) if d == 0 else zz(1 + k // 2)
            cols = pl.ds(ag_half(d, k) * half, half)
            spot = tok.at[block, :, cols]
            rcopy(spot, spot, ag_s.at[d, k], ag_r.at[d, k], z=zz(1)).wait_recv()
            if k + 2 < PER:
                ag_copy(d, k + 2).start()
        for j in {1: (0,), 2: (1, 2), 3: (3, 4), 4: (5,), 5: (6, 7)}.get(k, ()):
            hand_on(j)
        for j in {3: (0,), 4: (1, 2), 5: (3, 4), 6: (5,)}.get(k, ()):
            hand_over(j)
        if k == 1:
            q_copy.wait_recv()
            b_copy.wait_recv()
            bias[:, own] = b_own[...].reshape(1, width)
            bias[:, far] = b_far[...].reshape(1, width)
            far_columns()
        if k in (1, 3):
            norm_block(zz(-1 - k // 2))
            norm_block(zz(1 + k // 2))
        if k == 4:
            local[6].wait()
            backward_chunk(0)
        if k == 5:
            first_hop(0)
            backward_chunk(1)
            first_hop(1)
            norm_block(zz(-3))
            norm_block(zz(3))
            backward_chunk(2)
            first_hop(2)
        if k == 6:
            backward_chunk(3)
            first_hop(3)
            norm_block(zz(4))

    def event(e, carry):
        r = lax.rem(e, 16)
        hop = r // 4
        c = e // 16 * 4 + lax.rem(r, 4)

        @pl.when((hop == 0) & (e < 32))
        def _():
            first_hop(c)

        @pl.when((hop > 0) & (e < 32))
        def _():
            later_hop(c, hop)

        @pl.when((e == 5) | (e == 7))
        def _():
            hand_over(6 + (e - 5) // 2)

        @pl.when(e < 12)
        def _():
            c = 4 + (e - 4) // 2
            odd = lax.rem(e, 2)

            @pl.when(odd == 0)
            def _():
                weights_here(c)
            backward_part(c, odd * (F // bt // 2), F // bt // 2)

        @pl.when((e >= 8) & (e < 16))
        def _():
            c = e - 8
            gain_part(c)

            @pl.when(c != z)
            def _():
                g_send(c).start()

        @pl.when((e >= 12) & (e < 32))
        def _():
            forward_quarter((e - 12) // 4, lax.rem(e, 4))

        @pl.when(e == 21)
        def _():
            total = gp[z]
            for k in range(1, Z):
                spot = gr.at[zz(k)]
                rcopy(spot, spot, g_s.at[zz(k)], g_r.at[zz(k)], z=zz(1)).wait_recv()
                total = total + gr[zz(k)]
            gs[...] = total
            gy_copy.start()

        @pl.when(e == 24)
        def _():
            o_copy.start()

        @pl.when(e == 25)
        def _():
            gy_copy.wait_recv()
            gf[z] = gs[...] + gy[...]
            for k in range(1, Z):
                gf_send(k).start()

        @pl.when((e >= 24) & (e < 32))
        def _():
            c = e - 24
            for k in range(2):
                w_copy(c, k).wait_send()
                x_copy(c, k).wait_send()
                d_copy(c, k).wait_send()

            @pl.when(c != z)
            def _():
                g_send(c).wait_send()

        @pl.when(e >= 28)
        def _():
            c = e - 28
            for d in range(2):
                for slot in range(PER):
                    rs_copy(d, c, slot, rb.at[d, c, slot]).wait_send()

        @pl.when(e == 28)
        def _():
            for d in range(2):
                for k in range(PER):
                    ag_copy(d, k).wait_send()
            q_copy.wait_send()
            b_copy.wait_send()
            gy_copy.wait_send()

        @pl.when(e == 32)
        def _():
            o_local.start()

        @pl.when(e == 33)
        def _():
            for k in range(1, Z):
                spot = gf.at[zz(k)]
                rcopy(spot, spot, gf_s.at[k], gf_r.at[zz(k)], z=zz(1)).wait_recv()
            g_out.start()

        @pl.when(((e >= 24) & (e < 28)) | (e >= 32))
        def _():
            finish(jnp.where(e < 28, e - 24, e - 28))
        return carry

    lax.fori_loop(4, 36, event, 0)
    mean = jnp.sum(inner[...], axis=1, keepdims=True) / dim
    s = scl[z]
    st[0] = s
    st[1] = s * s * s * jnp.broadcast_to(mean, s.shape)
    st_copy = pltpu.make_async_copy(st, st_o, loc.at[9])
    st_copy.start()
    for k in range(1, Z):
        gf_send(k).wait_send()
    bg_copy.wait()
    o_copy.wait()
    o_local.wait()
    g_out.wait()
    for c in range(N):
        ng_copy(c).wait()
    st_copy.wait()


def settle(
    qkv_i, ng_i, st_i, gg_i, bg_i, tok_h, gain_h, qkv_o, tg_o, gg_o, bg_o,
    qkv, ng, st, gg, bg, tok, gain, sem_i, sem_o, ng_s, tg_s,
):
    rows, dim = ng.shape
    parts = ng_s.shape[0]
    wide = dim // parts
    half = qkv.shape[0] // 2

    def loads():
        yield pltpu.make_async_copy(st_i, st, sem_i.at[0])
        yield pltpu.make_async_copy(gain_h, gain, sem_i.at[1])
        yield pltpu.make_async_copy(tok_h, tok, sem_i.at[2])

    first = list(loads())
    for copy in first:
        copy.start()
    pieces = []
    for q in range(parts):
        at = pl.ds(q * wide, wide)
        copy = pltpu.make_async_copy(ng_i.at[:, at], ng.at[:, at], ng_s.at[q])
        copy.start()
        pieces.append(copy)
    through = []
    for k, (src, mid, dst) in enumerate((
        (qkv_i.at[pl.ds(0, half)], qkv.at[pl.ds(0, half)], qkv_o.at[pl.ds(0, half)]),
        (qkv_i.at[pl.ds(half, half)], qkv.at[pl.ds(half, half)], qkv_o.at[pl.ds(half, half)]),
        (gg_i, gg, gg_o),
        (bg_i, bg, bg_o),
    )):
        copy = pltpu.make_async_copy(src, mid, sem_i.at[3 + k])
        copy.start()
        through.append((copy, pltpu.make_async_copy(mid, dst, sem_o.at[k])))
    for copy in first:
        copy.wait()
    step = 512
    s = jnp.concatenate([st[0]] * (step // 128), axis=1)
    k = jnp.concatenate([st[1]] * (step // 128), axis=1)
    sent = []
    for q in range(parts):
        pieces[q].wait()

        def one(i, carry):
            at = pl.ds(pl.multiple_of(q * wide + i * step, step), step)
            ng[:, at] = s * gain[:, at] * ng[:, at] - tok[:, at].astype(f32) * k
            return carry

        lax.fori_loop(0, wide // step, one, 0)
        at = pl.ds(q * wide, wide)
        copy = pltpu.make_async_copy(ng.at[:, at], tg_o.at[:, at], tg_s.at[q])
        copy.start()
        sent.append(copy)
        got, put = through[q]
        got.wait()
        put.start()
        sent.append(put)
    for copy in sent:
        copy.wait()


def tables(tokens_per):
    mp = 2 * Z
    block = np.arange(mp).reshape(Z, 2).T.reshape(-1)
    position = (block[:, None] * (SEQ_LEN // mp) + np.arange(tokens_per)[None, :]).reshape(-1)
    half = HEAD // 2
    inverse = np.exp(-np.log(1000000.0) * (2.0 * np.arange(half) / HEAD))
    angle = position[:, None].astype(np.float64) * inverse[None, :]
    c, s = np.cos(angle), np.sin(angle)
    shape = (2, Z * tokens_per, HEAD)
    return (
        np.concatenate([c, c], axis=1).astype(np.float32).reshape(shape),
        np.concatenate([-s, s], axis=1).astype(np.float32).reshape(shape),
    )


def shards(tokens, norm_gain, qkv_weight, qkv_bias, qkv_grad):
    rows, dim = tokens.shape
    width = qkv_weight.shape[1]
    F = dim // N
    H = F // 2
    both = 2 * width
    cos, sin = tables(rows)
    any_spec = pl.BlockSpec(memory_space=pl.ANY)
    dma = pltpu.SemaphoreType.DMA
    V = pltpu.VMEM
    raw = pl.pallas_call(
        kernel,
        name="qkv_ring",
        out_shape=(
            jax.ShapeDtypeStruct((Z, 2, rows, width), bf16),
            jax.ShapeDtypeStruct((rows, dim), f32),
            jax.ShapeDtypeStruct((2, rows, 128), f32),
            jax.ShapeDtypeStruct((Z, 1, F), f32),
            jax.ShapeDtypeStruct((width,), f32),
        ),
        in_specs=[any_spec] * 7,
        out_specs=(any_spec,) * 5,
        scratch_shapes=[
            V((dim, both), bf16),
            V((Z, rows, dim), bf16),
            V((Z, rows, dim), bf16),
            V((Z, rows, dim), f32),
            V((2, N, PER, rows, H), bf16),
            V((2, N, 2, rows, H), bf16),
            V((Z, 2, rows, width), bf16),
            V((Z, rows, width), bf16),
            V((Z * rows, both), bf16),
            V((Z, rows, both), bf16),
            V((rows, dim), f32),
            V((2, rows, 128), f32),
            V((Z, rows, 128), f32),
            V((rows, 128), f32),
            V((Z * rows, 256), f32),
            V((N, 1, F), f32),
            V((Z, 1, F), f32),
            V((1, F), f32),
            V((1, F), f32),
            V((Z, 1, F), f32),
            V((1, dim), f32),
            V((1, both), f32),
            V((width,), f32),
            V((width,), f32),
            V((1, width), f32),
            V((width,), f32),
            V(cos.shape, f32),
            V(sin.shape, f32),
            dma((2, PER)), dma((2, PER)),
            dma((2, N)), dma((2, N)),
            dma((2, N)), dma((2, N)),
            dma((2, N)), dma((2, N)),
            dma((2, N, PER)), dma((2, N, PER)),
            dma((1,)), dma((1,)),
            dma((1,)), dma((1,)),
            dma((1,)), dma((1,)),
            dma((Z,)), dma((Z,)),
            dma((1,)), dma((1,)),
            dma((Z,)), dma((Z,)),
            dma((N,)),
            dma((14,)),
        ],
        compiler_params=pltpu.CompilerParams(
            collective_id=0, has_side_effects=True, vmem_limit_bytes=66_000_000
        ),
    )(
        tokens,
        qkv_weight,
        qkv_grad.reshape(Z, 2, rows, width),
        norm_gain.reshape(1, dim),
        qkv_bias,
        jnp.asarray(cos),
        jnp.asarray(sin),
    )
    qkv, tokens_grad, gain_grad, bias_grad = pl.pallas_call(
        settle,
        name="settle",
        out_shape=(
            jax.ShapeDtypeStruct((Z, 2, rows, width), bf16),
            jax.ShapeDtypeStruct((rows, dim), f32),
            jax.ShapeDtypeStruct((Z, 1, F), f32),
            jax.ShapeDtypeStruct((width,), f32),
        ),
        in_specs=[any_spec] * 7,
        out_specs=(any_spec,) * 4,
        scratch_shapes=[
            V((Z, 2, rows, width), bf16),
            V((rows, dim), f32),
            V((2, rows, 128), f32),
            V((Z, 1, F), f32),
            V((width,), f32),
            V((rows, dim), bf16),
            V((1, dim), f32),
            dma((7,)), dma((4,)), dma((4,)), dma((4,)),
        ],
        compiler_params=pltpu.CompilerParams(vmem_limit_bytes=66_000_000),
    )(*raw, tokens, norm_gain.reshape(1, dim))
    return (
        qkv.reshape(2 * Z * rows, width),
        tokens_grad,
        gain_grad.reshape(dim),
        bias_grad,
    )


def solution(mesh):
    dp, mp = AXES[:3], AXES[3:]
    split = Mesh(mesh.devices.reshape(2, mesh.shape["dp"] // 4, 2, Z, 2), AXES)
    return jax.shard_map(
        shards,
        mesh=split,
        in_specs=(P(AXES, None), P(), P(None, mp), P(mp), P(dp, mp)),
        out_specs=(P(dp, mp), P(AXES, None), P(dp), P(AXES)),
        check_vma=False,
    )
```

```python
import functools

import jax
import jax.numpy as jnp
import numpy as np
from jax import lax
from jax.experimental import pallas as pl
from jax.experimental.pallas import tpu as pltpu
from jax.sharding import Mesh
from jax.sharding import PartitionSpec as P

HEAD = 128
SEQ_LEN = 32768
MESH = pl.DeviceIdType.MESH
AXES = ("yh", "x", "core", "z", "yl")
Z = 8
N = 8
PER = 7
f32 = jnp.float32
bf16 = jnp.bfloat16


def rcopy(src, dst, ssem, rsem, **where):
    return pltpu.make_async_remote_copy(
        src_ref=src, dst_ref=dst, send_sem=ssem, recv_sem=rsem, device_id=where, device_id_type=MESH
    )


def kernel(
    tok_h, w_h, qg_h, gain_h, bias_h, cos_h, sin_h,
    qkv_o, ng_o, st_o, gg_o, bg_o,
    w, tok, nrm, part, rb, sb, qb, qp, jl, out, ng, st, scl, inner, acc,
    gp, gr, gy, gf, gain, bias, b_own, b_far, bgv, bg1, cosv, sinv,
    ag_r, ag_s, w_r, w_s, x_r, d_r, rs_r, rs_s, q_r, q_s, b_r, b_s, o_r, o_s,
    g_r, g_s, gy_r, gy_s, gf_r, gf_s, gl_r, gl_s, ng_s, loc,
):
    rows, dim = tok_h.shape
    width = w_h.shape[1]
    F = dim // N
    H = F // 2
    half = dim // 2
    yh, x, core, z, yl = (lax.axis_index(a) for a in AXES)

    def zz(k):
        return lax.rem(z + (k + Z), Z)

    direct = {"yl": 1 - yl}
    other = {"yh": 1 - yh, "yl": 1 - yl}
    sibling = {"core": 1 - core}
    nx = lax.axis_size("x")
    beside = [{"x": lax.rem(x + 1, nx)}, {"x": lax.rem(x + nx - 1, nx)}]
    side = lax.rem(x, 2)
    own = pl.ds(pl.multiple_of(yl * width, 128), width)
    far = pl.ds(pl.multiple_of((1 - yl) * width, 128), width)

    local = [
        pltpu.make_async_copy(tok_h, tok.at[z], loc.at[0]),
        pltpu.make_async_copy(qg_h, qb, loc.at[1]),
        pltpu.make_async_copy(cos_h, cosv, loc.at[2]),
        pltpu.make_async_copy(sin_h, sinv, loc.at[3]),
        pltpu.make_async_copy(gain_h, gain, loc.at[4]),
        pltpu.make_async_copy(bias_h, b_own, loc.at[5]),
        pltpu.make_async_copy(w_h, w.at[:, own], loc.at[6]),
    ]
    for copy in local:
        copy.start()

    barrier = pltpu.get_barrier_semaphore()
    for where in ({"z": zz(1)}, {"z": zz(-1)}, direct, other, sibling, *beside):
        pl.semaphore_signal(barrier, inc=1, device_id=where, device_id_type=MESH)
    pl.semaphore_wait(barrier, 7)
    local[0].wait()

    def ag_half(d, k):
        return d if k % 2 == 0 else 1 - d

    def ag_copy(d, k):
        step = k // 2
        block = zz(-step) if d == 0 else zz(step)
        cols = pl.ds(ag_half(d, k) * half, half)
        spot = tok.at[block, :, cols]
        return rcopy(spot, spot, ag_s.at[0], ag_r.at[k], z=zz(1 if d == 0 else -1))

    for k in range(2):
        for d in range(2):
            ag_copy(d, k).start()

    q_copy = rcopy(qg_h.at[:, 1 - yl], qp, q_s.at[0], q_r.at[0], **direct)
    q_copy.start()
    b_copy = rcopy(bias_h, b_far, b_s.at[0], b_r.at[0], **direct)
    b_copy.start()

    piece = F // 8

    def w_rows(j, par, who, s, n):
        return pl.ds(pl.multiple_of(j * F + par * 4 * piece + who * 2 * piece + s * piece, piece), n * piece)

    def w_copy(j, s):
        at = w_rows(j, side, core, s, 1)
        return rcopy(w_h.at[at], w.at[at, own], w_s.at[0], w_r.at[j], **(direct if s == 0 else other))

    def w_got(j):
        spot = w.at[w_rows(j, side, core, 0, 2), far]
        return rcopy(spot, spot, w_s.at[0], w_r.at[j], **direct)

    def x_copy(j, s):
        spot = w.at[w_rows(j, side, core, s, 1), far]
        return rcopy(spot, spot, w_s.at[0], x_r.at[j], **beside[s])

    def x_got(j):
        spot = w.at[w_rows(j, 1 - side, core, 0, 2), far]
        return rcopy(spot, spot, w_s.at[0], x_r.at[j], **beside[0])

    def d_copy(j, k):
        spot = w.at[w_rows(j, side if k == 0 else 1 - side, core, 0, 2), far]
        return rcopy(spot, spot, w_s.at[0], d_r.at[j], **sibling)

    def hand_on(j):
        w_got(j).wait_recv()
        for s in range(2):
            x_copy(j, s).start()
        d_copy(j, 0).start()

    def hand_over(j):
        x_got(j).wait_recv()
        d_copy(j, 1).start()

    for j in range(N):
        w_copy(j, 0).start()
        w_copy(j, 1).start()

    def norm_block(b):
        step = min(512, dim)

        def sq(i, total):
            v = tok[b, :, pl.ds(pl.multiple_of(i * step, step), step)].astype(f32)
            v = v * v
            for q in range(step // 128):
                total = total + v[:, q * 128:(q + 1) * 128]
            return total

        total = lax.fori_loop(0, dim // step, sq, jnp.zeros((rows, 128), f32))
        mean = jnp.sum(total, axis=1, keepdims=True) / dim
        s = jnp.broadcast_to(lax.rsqrt(mean + 1e-06), (rows, 128))
        scl[b] = s
        wide = jnp.concatenate([s] * (step // 128), axis=1)

        def put(i, carry):
            at = pl.ds(pl.multiple_of(i * step, step), step)
            v = tok[b, :, at].astype(f32)
            nrm[b, :, at] = (v * wide * gain[:, at]).astype(bf16)
            return carry

        lax.fori_loop(0, dim // step, put, 0)

    def turn_back(x, line, b, is_value):
        c = cosv[line, pl.ds(pl.multiple_of(b * rows, rows), rows), :]
        s = sinv[line, pl.ds(pl.multiple_of(b * rows, rows), rows), :]
        r = x * c - pltpu.roll(x, HEAD // 2, 1) * s
        return r if is_value is None else jnp.where(is_value, x, r)

    heads = width // HEAD

    def own_columns():
        def one(b, sums):
            at = pl.ds(pl.multiple_of(b * rows, rows), rows)
            new = []
            for h in range(heads):
                value = (yl == 1) if h == heads - 1 else None
                hs = pl.ds(h * HEAD, HEAD)
                r = turn_back(qb[b, yl, :, hs].astype(f32), yl, b, value)
                jl[at, pl.ds(pl.multiple_of(yl * width + h * HEAD, HEAD), HEAD)] = r.astype(bf16)
                r = r + turn_back(qb[b, 1 - yl, :, hs].astype(f32), 1 - yl, b, value)
                total = sums[h]
                for q in range(rows // 8):
                    total = total + r[q * 8:(q + 1) * 8]
                new.append(total)
            return tuple(new)

        sums = lax.fori_loop(0, Z, one, (jnp.zeros((8, HEAD), f32),) * heads)
        for h in range(heads):
            bgv[:, h * HEAD:(h + 1) * HEAD] = jnp.sum(sums[h], axis=0, keepdims=True)

    def far_columns():
        def one(b, carry):
            at = pl.ds(pl.multiple_of(b * rows, rows), rows)
            for h in range(heads):
                value = (yl == 0) if h == heads - 1 else None
                r = turn_back(qp[b, :, pl.ds(h * HEAD, HEAD)].astype(f32), yl, b, value)
                jl[at, pl.ds(pl.multiple_of((1 - yl) * width + h * HEAD, HEAD), HEAD)] = r.astype(bf16)
            return carry

        lax.fori_loop(0, Z, one, 0)

    bt = min(256, F)

    def backward_part(c, first, count):
        def one(t, carry):
            at = pl.ds(pl.multiple_of(c * F + t * bt, bt), bt)
            got = lax.dot_general(jl[...], w[at, :], (((1,), (1,)), ((), ())), preferred_element_type=f32)
            part[:, :, at] = got.reshape(Z, rows, bt)
            return carry

        lax.fori_loop(first, first + count, one, 0)

    def weights_here(c):
        spot = w.at[w_rows(c, 0, 0, 0, 4), far]
        rcopy(spot, spot, w_s.at[0], d_r.at[c], **sibling).wait_recv()

    def backward_chunk(c):
        weights_here(c)
        backward_part(c, 0, F // bt)

    def span(c, hf):
        return pl.ds(pl.multiple_of(c * F + hf * H, H), H)

    def rs_copy(d, c, slot, src):
        return rcopy(src, rb.at[d, c, slot], rs_s.at[0], rs_r.at[lax.rem(c, 4), slot], z=zz(1 if d == 0 else -1))

    def rs_wait(c, slot):
        spot = rb.at[:, c, slot]
        rcopy(spot, spot, rs_s.at[0], rs_r.at[lax.rem(c, 4), slot], z=zz(1)).wait_recv()

    def first_hop(c):
        for d in range(2):
            for short in range(2):
                hf = d if short == 0 else 1 - d
                dist = 4 - short
                sb[d, c, short] = part[zz(dist if d == 0 else -dist), :, span(c, hf)].astype(bf16)
                rs_copy(d, c, 4 * short, sb.at[d, c, short]).start()

    def pass_on(c, hop, short):
        slot = 4 * short + hop - 1
        rs_wait(c, slot)
        for d in range(2):
            hf = short if d == 0 else 1 - short
            dist = 4 - hop - short
            mine = part[zz(dist if d == 0 else -dist), :, span(c, hf)]
            rb[d, c, slot] = (rb[d, c, slot].astype(f32) + mine).astype(bf16)
            rs_copy(d, c, slot + 1, rb.at[d, c, slot]).start()

    def ng_copy(c):
        at = pl.ds(pl.multiple_of(c * F, F), F)
        return pltpu.make_async_copy(ng.at[:, at], ng_o.at[:, at], ng_s.at[0])

    def finish(c):
        rs_wait(c, 3)
        rs_wait(c, 6)
        total = inner[...]
        for hf in range(2):
            at = span(c, hf)
            got = part[z, :, at] + rb[hf, c, 3].astype(f32) + rb[1 - hf, c, 6].astype(f32)
            ng[:, at] = got
            t = got * gain[:, at] * tok[z, :, at].astype(f32)
            for q in range(H // 128):
                total = total + t[:, q * 128:(q + 1) * 128]
        inner[...] = total
        ng_copy(c).start()

    def gain_part(c):
        def one(t, carry):
            per = H // 128
            at = pl.ds(pl.multiple_of(c * F + t * 128, 128), 128)
            total = jnp.zeros((rows, 128), f32)
            for b in range(Z):
                total = total + part[b, :, at] * tok[b, :, at].astype(f32) * scl[b]
            spot = pl.ds(pl.multiple_of(lax.rem(t, per) * 128, 128), 128)
            gp[c, t // per, :, spot] = jnp.sum(total, axis=0, keepdims=True)
            return carry

        lax.fori_loop(0, F // 128, one, 0)

    def gy_send(c):
        return rcopy(gp.at[c, 1 - yl], gy.at[c], gy_s.at[0], gy_r.at[0], **direct)

    def g_send(c):
        return rcopy(gp.at[c, yl], gr.at[z], g_s.at[0], g_r.at[0], z=c)

    def gf_send(k):
        return rcopy(gf.at[yl, z], gf.at[yl, z], gf_s.at[0], gf_r.at[0], z=zz(k))

    gl_copy = rcopy(gf.at[yl], gf.at[yl], gl_s.at[0], gl_r.at[0], **direct)
    g_out = [pltpu.make_async_copy(gf.at[h], gg_o.at[:, h], loc.at[10 + h]) for h in range(2)]

    def forward_quarter(t, k):
        n = jnp.where(yl == 0, t, 4 - t)
        cols = pl.ds(pl.multiple_of(n * 256, 256), 256)
        deep = dim // 4

        @pl.when(k == 0)
        def _():
            acc[...] = jnp.broadcast_to(bias[:, cols], acc.shape)

        at = pl.ds(pl.multiple_of(k * deep, deep), deep)
        lhs = nrm[:, :, at].reshape(Z * rows, deep)
        acc[...] += jnp.dot(lhs, w[at, cols], preferred_element_type=f32)

        @pl.when(k == 3)
        def _():
            for b in range(Z):
                at = pl.ds(b * rows, rows)
                for h in range(2):
                    x = acc[at, h * HEAD:(h + 1) * HEAD]
                    r = x * cosv[yl, at, :] + pltpu.roll(x, HEAD // 2, 1) * sinv[yl, at, :]
                    if h == 1:
                        r = jnp.where(n == 4, x, r)
                    out[b, :, pl.ds(pl.multiple_of(n * 256 + h * HEAD, HEAD), HEAD)] = r.astype(bf16)

    def o_copy(p):
        start = ((width, width - 128), (width + 128, 256), (width + 384, 0))[p]
        n = 128 if p == 0 else 256
        src = pl.multiple_of(jnp.where(yl == 0, start[0], start[1]), 128)
        dst = pl.multiple_of(src - (1 - yl) * width, 128)
        return rcopy(out.at[:, :, pl.ds(src, n)], qkv_o.at[:, yl, :, pl.ds(dst, n)], o_s.at[0], o_r.at[0], **direct)

    o_local = pltpu.make_async_copy(out.at[:, :, own], qkv_o.at[:, yl], loc.at[8])

    inner[...] = jnp.zeros_like(inner)

    for k in range(1, 5):
        local[k].wait()
    own_columns()
    norm_block(z)
    local[5].wait()
    bg1[...] = bgv[...].reshape(width)
    bg_copy = pltpu.make_async_copy(bg1, bg_o, loc.at[7])
    bg_copy.start()

    for k in range(PER):
        rcopy(tok.at[z], tok.at[z], ag_s.at[0], ag_r.at[k], z=zz(1)).wait_recv()
        for d in range(2):
            if k + 2 < PER:
                ag_copy(d, k + 2).start()
        for j in {1: (0,), 2: (1, 2), 3: (3, 4), 4: (5,), 5: (6, 7)}.get(k, ()):
            hand_on(j)
        for j in {3: (0,), 4: (1, 2), 5: (3, 4), 6: (5,)}.get(k, ()):
            hand_over(j)
        if k == 1:
            q_copy.wait_recv()
            b_copy.wait_recv()
            bias[:, own] = b_own[...].reshape(1, width)
            bias[:, far] = b_far[...].reshape(1, width)
            far_columns()
        if k == 4:
            local[6].wait()
            for c in range(3):
                backward_chunk(c)
        if k == 5:
            for c in range(3):
                first_hop(c)
        if k in (1, 3, 5):
            norm_block(zz(-1 - k // 2))
            norm_block(zz(1 + k // 2))
        if k == 5:
            backward_chunk(3)
            first_hop(3)
            backward_chunk(4)
        if k == 6:
            norm_block(zz(4))

    def event(e, carry):
        r = lax.rem(e, 16)
        base = e // 16 * 4
        hop = r // 4
        c = base + lax.rem(r, 4)

        @pl.when((hop == 0) & (e < 32))
        def _():
            first_hop(c)

        @pl.when(hop > 0)
        def _():
            j = lax.rem(r, 4)
            pair = base + 2 * lax.rem(j, 2)
            pass_on(jnp.where(hop == 2, pair, c), hop, jnp.where(hop == 2, j // 2, 0))

            @pl.when(hop < 3)
            def _():
                pass_on(jnp.where(hop == 2, pair + 1, c), hop, jnp.where(hop == 2, j // 2, 1))

        @pl.when((e == 4) | (e == 6))
        def _():
            hand_over(6 + (e - 4) // 2)

        @pl.when((e >= 5) & (e < 11))
        def _():
            c = 5 + (e - 5) // 2
            odd = lax.rem(e - 5, 2)

            @pl.when(odd == 0)
            def _():
                weights_here(c)
            backward_part(c, odd * (F // bt // 2), F // bt // 2)

        @pl.when((e < 9) | ((e >= 11) & (e < 14)))
        def _():
            c = jnp.where(e < 9, e - 4, e - 6)
            gain_part(c)
            gy_send(c).start()

        @pl.when(e == 17)
        def _():
            rcopy(gy, gy, gy_s.at[0], gy_r.at[0], **direct).wait()
            for c in range(N):
                gp[c, yl] = gp[c, yl] + gy[c]

                @pl.when(c != z)
                def _(c=c):
                    g_send(c).start()

        @pl.when((e >= 9) & (e < 29))
        def _():
            forward_quarter((e - 9) // 4, lax.rem(e - 9, 4))

        for p, when in enumerate((20, 24, 28)):
            @pl.when(e == when)
            def _(p=p):
                o_copy(p).start()

        @pl.when(e == 24)
        def _():
            total = gp[z, yl]
            spot = gr.at[pl.ds(0, Z - 1)]
            rcopy(spot, spot, g_s.at[0], g_r.at[0], z=zz(1)).wait()
            for k in range(1, Z):
                total = total + gr[zz(k)]
            gf[yl, z] = total
            for k in range(1, Z):
                gf_send(k).start()

        @pl.when(e == 29)
        def _():
            spot = gf.at[0, pl.ds(0, Z - 1)]
            rcopy(spot, spot, gf_s.at[0], gf_r.at[0], z=zz(1)).wait()
            gl_copy.start()

        @pl.when(e == 32)
        def _():
            o_local.start()

        @pl.when(((e >= 18) & (e < 22)) | (e >= 32))
        def _():
            finish(jnp.where(e < 22, e - 18, e - 28))

        @pl.when(e == 25)
        def _():
            spot = tok.at[pl.ds(0, PER)]
            rcopy(spot, spot, ag_s.at[0], ag_r.at[0], z=zz(1)).wait_send()
            q_copy.wait_send()
            b_copy.wait_send()
            spot = w.at[:, own]
            rcopy(spot, spot, w_s.at[0], w_r.at[0], **direct).wait_send()

        @pl.when(e == 33)
        def _():
            gl_copy.wait_send()
            spot = gf.at[1 - yl]
            rcopy(spot, spot, gl_s.at[0], gl_r.at[0], **direct).wait_recv()
            for h in range(2):
                g_out[h].start()
        return carry

    lax.fori_loop(4, 36, event, 0)
    mean = jnp.sum(inner[...], axis=1, keepdims=True) / dim
    s = scl[z]
    st[0] = s
    st[1] = s * s * s * jnp.broadcast_to(mean, s.shape)
    st_copy = pltpu.make_async_copy(st, st_o, loc.at[9])
    st_copy.start()
    bg_copy.wait()
    rcopy(out.at[:, :, far], out.at[:, :, far], o_s.at[0], o_r.at[0], **direct).wait()
    rcopy(rb, rb, rs_s.at[0], rs_r.at[0, 0], z=zz(1)).wait_send()
    o_local.wait()
    for h in range(2):
        g_out[h].wait()
    pltpu.make_async_copy(ng, ng_o, ng_s.at[0]).wait()
    st_copy.wait()


def settle(
    qkv_i, ng_i, st_i, gg_i, bg_i, tok_h, gain_h, qkv_o, tg_o, gg_o, bg_o,
    qkv, ng, st, gg, bg, tok, gain, sem_i, sem_o, ng_s, tg_s,
):
    rows, dim = ng.shape
    parts = ng_s.shape[0]
    wide = dim // parts
    half = qkv.shape[0] // 2

    def loads():
        yield pltpu.make_async_copy(st_i, st, sem_i.at[0])
        yield pltpu.make_async_copy(gain_h, gain, sem_i.at[1])
        yield pltpu.make_async_copy(tok_h, tok, sem_i.at[2])

    first = list(loads())
    for copy in first:
        copy.start()
    pieces = []
    for q in range(parts):
        at = pl.ds(q * wide, wide)
        copy = pltpu.make_async_copy(ng_i.at[:, at], ng.at[:, at], ng_s.at[q])
        copy.start()
        pieces.append(copy)
    through = []
    for k, (src, mid, dst) in enumerate((
        (qkv_i.at[pl.ds(0, half)], qkv.at[pl.ds(0, half)], qkv_o.at[pl.ds(0, half)]),
        (qkv_i.at[pl.ds(half, half)], qkv.at[pl.ds(half, half)], qkv_o.at[pl.ds(half, half)]),
        (gg_i, gg, gg_o),
        (bg_i, bg, bg_o),
    )):
        copy = pltpu.make_async_copy(src, mid, sem_i.at[3 + k])
        copy.start()
        through.append((copy, pltpu.make_async_copy(mid, dst, sem_o.at[k])))
    for copy in first:
        copy.wait()
    step = 512
    s = jnp.concatenate([st[0]] * (step // 128), axis=1)
    k = jnp.concatenate([st[1]] * (step // 128), axis=1)
    sent = []
    for q in range(parts):
        pieces[q].wait()

        def one(i, carry):
            at = pl.ds(pl.multiple_of(q * wide + i * step, step), step)
            ng[:, at] = s * gain[:, at] * ng[:, at] - tok[:, at].astype(f32) * k
            return carry

        lax.fori_loop(0, wide // step, one, 0)
        at = pl.ds(q * wide, wide)
        copy = pltpu.make_async_copy(ng.at[:, at], tg_o.at[:, at], tg_s.at[q])
        copy.start()
        sent.append(copy)
        got, put = through[q]
        got.wait()
        put.start()
        sent.append(put)
    for copy in sent:
        copy.wait()


def tables(tokens_per):
    mp = 2 * Z
    block = np.arange(mp).reshape(Z, 2).T.reshape(-1)
    position = (block[:, None] * (SEQ_LEN // mp) + np.arange(tokens_per)[None, :]).reshape(-1)
    half = HEAD // 2
    inverse = np.exp(-np.log(1000000.0) * (2.0 * np.arange(half) / HEAD))
    angle = position[:, None].astype(np.float64) * inverse[None, :]
    c, s = np.cos(angle), np.sin(angle)
    shape = (2, Z * tokens_per, HEAD)
    return (
        np.concatenate([c, c], axis=1).astype(np.float32).reshape(shape),
        np.concatenate([-s, s], axis=1).astype(np.float32).reshape(shape),
    )


def shards(tokens, norm_gain, qkv_weight, qkv_bias, qkv_grad):
    rows, dim = tokens.shape
    width = qkv_weight.shape[1]
    F = dim // N
    H = F // 2
    both = 2 * width
    cos, sin = tables(rows)
    any_spec = pl.BlockSpec(memory_space=pl.ANY)
    dma = pltpu.SemaphoreType.DMA
    V = pltpu.VMEM
    raw = pl.pallas_call(
        kernel,
        name="qkv_ring",
        out_shape=(
            jax.ShapeDtypeStruct((Z, 2, rows, width), bf16),
            jax.ShapeDtypeStruct((rows, dim), f32),
            jax.ShapeDtypeStruct((2, rows, 128), f32),
            jax.ShapeDtypeStruct((Z, 2, 1, H), f32),
            jax.ShapeDtypeStruct((width,), f32),
        ),
        in_specs=[any_spec] * 7,
        out_specs=(any_spec,) * 5,
        scratch_shapes=[
            V((dim, both), bf16),
            V((Z, rows, dim), bf16),
            V((Z, rows, dim), bf16),
            V((Z, rows, dim), f32),
            V((2, N, PER, rows, H), bf16),
            V((2, N, 2, rows, H), bf16),
            V((Z, 2, rows, width), bf16),
            V((Z, rows, width), bf16),
            V((Z * rows, both), bf16),
            V((Z, rows, both), bf16),
            V((rows, dim), f32),
            V((2, rows, 128), f32),
            V((Z, rows, 128), f32),
            V((rows, 128), f32),
            V((Z * rows, 256), f32),
            V((N, 2, 1, H), f32),
            V((Z, 1, H), f32),
            V((N, 1, H), f32),
            V((2, Z, 1, H), f32),
            V((1, dim), f32),
            V((1, both), f32),
            V((width,), f32),
            V((width,), f32),
            V((1, width), f32),
            V((width,), f32),
            V(cos.shape, f32),
            V(sin.shape, f32),
            dma((PER,)), dma((1,)),
            dma((N,)), dma((1,)), dma((N,)), dma((N,)),
            dma((4, PER)), dma((1,)),
            dma((1,)), dma((1,)),
            dma((1,)), dma((1,)),
            dma((1,)), dma((1,)),
            dma((1,)), dma((1,)),
            dma((1,)), dma((1,)),
            dma((1,)), dma((1,)),
            dma((1,)), dma((1,)),
            dma((1,)),
            dma((14,)),
        ],
        compiler_params=pltpu.CompilerParams(
            collective_id=0, has_side_effects=True, vmem_limit_bytes=66_000_000
        ),
    )(
        tokens,
        qkv_weight,
        qkv_grad.reshape(Z, 2, rows, width),
        norm_gain.reshape(1, dim),
        qkv_bias,
        jnp.asarray(cos),
        jnp.asarray(sin),
    )
    qkv, tokens_grad, gain_grad, bias_grad = pl.pallas_call(
        settle,
        name="settle",
        out_shape=(
            jax.ShapeDtypeStruct((Z, 2, rows, width), bf16),
            jax.ShapeDtypeStruct((rows, dim), f32),
            jax.ShapeDtypeStruct((Z, 2, 1, H), f32),
            jax.ShapeDtypeStruct((width,), f32),
        ),
        in_specs=[any_spec] * 7,
        out_specs=(any_spec,) * 4,
        scratch_shapes=[
            V((Z, 2, rows, width), bf16),
            V((rows, dim), f32),
            V((2, rows, 128), f32),
            V((Z, 2, 1, H), f32),
            V((width,), f32),
            V((rows, dim), bf16),
            V((1, dim), f32),
            dma((7,)), dma((4,)), dma((4,)), dma((4,)),
        ],
        compiler_params=pltpu.CompilerParams(vmem_limit_bytes=66_000_000),
    )(*raw, tokens, norm_gain.reshape(1, dim))
    return (
        qkv.reshape(2 * Z * rows, width),
        tokens_grad,
        gain_grad.reshape(dim),
        bias_grad,
    )


def solution(mesh):
    dp, mp = AXES[:3], AXES[3:]
    split = Mesh(mesh.devices.reshape(2, mesh.shape["dp"] // 4, 2, Z, 2), AXES)
    return jax.shard_map(
        shards,
        mesh=split,
        in_specs=(P(AXES, None), P(), P(None, mp), P(mp), P(dp, mp)),
        out_specs=(P(dp, mp), P(AXES, None), P(dp), P(AXES)),
        check_vma=False,
    )
```

```python
import functools

import jax
import jax.numpy as jnp
import numpy as np
from jax import lax
from jax.experimental import pallas as pl
from jax.experimental.pallas import tpu as pltpu
from jax.sharding import Mesh
from jax.sharding import PartitionSpec as P

HEAD = 128
SEQ_LEN = 32768
MESH = pl.DeviceIdType.MESH
AXES = ("yh", "x", "core", "z", "yl")
Z = 8
N = 8
PER = 7
f32 = jnp.float32
bf16 = jnp.bfloat16


def rcopy(src, dst, ssem, rsem, **where):
    return pltpu.make_async_remote_copy(
        src_ref=src, dst_ref=dst, send_sem=ssem, recv_sem=rsem, device_id=where, device_id_type=MESH
    )


def kernel(
    tok_h, w_h, qg_h, gain_h, bias_h, cos_h, sin_h,
    qkv_o, ng_o, st_o, gg_o, bg_o,
    w, tok, nrm, part, rb, sb, qb, qp, jl, out, ng, st, scl, inner, acc,
    gp, gr, gy, gf, gain, bias, b_own, b_far, bgv, bg1, cosv, sinv,
    ag_r, ag_s, w_r, w_s, x_r, d_r, rs_r, rs_s, q_r, q_s, b_r, b_s, o_r, o_s,
    g_r, g_s, gy_r, gy_s, gf_r, gf_s, gl_r, gl_s, ng_s, loc,
):
    rows, dim = tok_h.shape
    width = w_h.shape[1]
    F = dim // N
    H = F // 2
    half = dim // 2
    yh, x, core, z, yl = (lax.axis_index(a) for a in AXES)

    def zz(k):
        return lax.rem(z + (k + Z), Z)

    direct = {"yl": 1 - yl}
    other = {"yh": 1 - yh, "yl": 1 - yl}
    sibling = {"core": 1 - core}
    nx = lax.axis_size("x")
    beside = [{"x": lax.rem(x + 1, nx)}, {"x": lax.rem(x + nx - 1, nx)}]
    side = lax.rem(x, 2)
    own = pl.ds(pl.multiple_of(yl * width, 128), width)
    far = pl.ds(pl.multiple_of((1 - yl) * width, 128), width)

    local = [
        pltpu.make_async_copy(tok_h, tok.at[z], loc.at[0]),
        pltpu.make_async_copy(qg_h, qb, loc.at[1]),
        pltpu.make_async_copy(cos_h, cosv, loc.at[2]),
        pltpu.make_async_copy(sin_h, sinv, loc.at[3]),
        pltpu.make_async_copy(gain_h, gain, loc.at[4]),
        pltpu.make_async_copy(bias_h, b_own, loc.at[5]),
        pltpu.make_async_copy(w_h, w.at[:, own], loc.at[6]),
    ]
    for copy in local:
        copy.start()

    barrier = pltpu.get_barrier_semaphore()
    for where in ({"z": zz(1)}, {"z": zz(-1)}, direct, other, sibling, *beside):
        pl.semaphore_signal(barrier, inc=1, device_id=where, device_id_type=MESH)
    pl.semaphore_wait(barrier, 7)
    local[0].wait()

    def ag_half(d, k):
        return d if k % 2 == 0 else 1 - d

    def ag_copy(d, k):
        step = k // 2
        block = zz(-step) if d == 0 else zz(step)
        cols = pl.ds(ag_half(d, k) * half, half)
        spot = tok.at[block, :, cols]
        return rcopy(spot, spot, ag_s.at[0], ag_r.at[k], z=zz(1 if d == 0 else -1))

    for k in range(2):
        for d in range(2):
            ag_copy(d, k).start()

    q_copy = rcopy(qg_h.at[:, 1 - yl], qp, q_s.at[0], q_r.at[0], **direct)
    b_copy = rcopy(bias_h, b_far, b_s.at[0], b_r.at[0], **direct)

    piece = F // 8

    cut = 7 * piece // 8

    def w_rows(j, par, who, s, n):
        first = j * F + par * 4 * piece + who * 2 * piece
        if n > 1:
            return pl.ds(pl.multiple_of(first, 2 * piece), n * piece)
        return pl.ds(pl.multiple_of(first + s * cut, 16), cut if s == 0 else 2 * piece - cut)

    def w_copy(j, s):
        at = w_rows(j, side, core, s, 1)
        return rcopy(w_h.at[at], w.at[at, own], w_s.at[0], w_r.at[j], **(direct if s == 0 else other))

    def w_got(j):
        spot = w.at[w_rows(j, side, core, 0, 2), far]
        return rcopy(spot, spot, w_s.at[0], w_r.at[j], **direct)

    def x_copy(j, s):
        spot = w.at[w_rows(j, side, core, 0, 2), far].at[pl.ds(s * piece, piece)]
        return rcopy(spot, spot, w_s.at[0], x_r.at[j], **beside[s])

    def x_got(j):
        spot = w.at[w_rows(j, 1 - side, core, 0, 2), far]
        return rcopy(spot, spot, w_s.at[0], x_r.at[j], **beside[0])

    def d_copy(j, k):
        spot = w.at[w_rows(j, side if k == 0 else 1 - side, core, 0, 2), far]
        return rcopy(spot, spot, w_s.at[0], d_r.at[j], **sibling)

    def hand_on(j):
        w_got(j).wait_recv()
        for s in range(2):
            x_copy(j, s).start()
        d_copy(j, 0).start()

    def hand_over(j):
        x_got(j).wait_recv()
        d_copy(j, 1).start()

    for j in range(N):
        if j == 4:
            b_copy.start()
            q_copy.start()
        w_copy(j, 0).start()
        w_copy(j, 1).start()

    def norm_block(b):
        step = min(512, dim)

        def sq(i, total):
            v = tok[b, :, pl.ds(pl.multiple_of(i * step, step), step)].astype(f32)
            v = v * v
            for q in range(step // 128):
                total = total + v[:, q * 128:(q + 1) * 128]
            return total

        total = lax.fori_loop(0, dim // step, sq, jnp.zeros((rows, 128), f32))
        mean = jnp.sum(total, axis=1, keepdims=True) / dim
        s = jnp.broadcast_to(lax.rsqrt(mean + 1e-06), (rows, 128))
        scl[b] = s
        wide = jnp.concatenate([s] * (step // 128), axis=1)

        def put(i, carry):
            at = pl.ds(pl.multiple_of(i * step, step), step)
            v = tok[b, :, at].astype(f32)
            nrm[b, :, at] = (v * wide * gain[:, at]).astype(bf16)
            return carry

        lax.fori_loop(0, dim // step, put, 0)

    def turn_back(x, line, b, is_value):
        c = cosv[line, pl.ds(pl.multiple_of(b * rows, rows), rows), :]
        s = sinv[line, pl.ds(pl.multiple_of(b * rows, rows), rows), :]
        r = x * c - pltpu.roll(x, HEAD // 2, 1) * s
        return r if is_value is None else jnp.where(is_value, x, r)

    heads = width // HEAD

    def own_columns():
        def one(b, sums):
            at = pl.ds(pl.multiple_of(b * rows, rows), rows)
            new = []
            for h in range(heads):
                value = (yl == 1) if h == heads - 1 else None
                hs = pl.ds(h * HEAD, HEAD)
                r = turn_back(qb[b, yl, :, hs].astype(f32), yl, b, value)
                jl[at, pl.ds(pl.multiple_of(yl * width + h * HEAD, HEAD), HEAD)] = r.astype(bf16)
                r = r + turn_back(qb[b, 1 - yl, :, hs].astype(f32), 1 - yl, b, value)
                total = sums[h]
                for q in range(rows // 8):
                    total = total + r[q * 8:(q + 1) * 8]
                new.append(total)
            return tuple(new)

        sums = lax.fori_loop(0, Z, one, (jnp.zeros((8, HEAD), f32),) * heads)
        for h in range(heads):
            bgv[:, h * HEAD:(h + 1) * HEAD] = jnp.sum(sums[h], axis=0, keepdims=True)

    def far_columns():
        def one(b, carry):
            at = pl.ds(pl.multiple_of(b * rows, rows), rows)
            for h in range(heads):
                value = (yl == 0) if h == heads - 1 else None
                r = turn_back(qp[b, :, pl.ds(h * HEAD, HEAD)].astype(f32), yl, b, value)
                jl[at, pl.ds(pl.multiple_of((1 - yl) * width + h * HEAD, HEAD), HEAD)] = r.astype(bf16)
            return carry

        lax.fori_loop(0, Z, one, 0)

    bt = min(256, F)

    def backward_part(c, first, count):
        def one(t, carry):
            at = pl.ds(pl.multiple_of(c * F + t * bt, bt), bt)
            got = lax.dot_general(jl[...], w[at, :], (((1,), (1,)), ((), ())), preferred_element_type=f32)
            part[:, :, at] = got.reshape(Z, rows, bt)
            return carry

        lax.fori_loop(first, first + count, one, 0)

    def weights_here(c):
        spot = w.at[w_rows(c, 0, 0, 0, 4), far]
        rcopy(spot, spot, w_s.at[0], d_r.at[c], **sibling).wait_recv()

    def backward_chunk(c):
        weights_here(c)
        backward_part(c, 0, F // bt)

    def span(c, hf):
        return pl.ds(pl.multiple_of(c * F + hf * H, H), H)

    def rs_copy(d, c, slot, src):
        return rcopy(src, rb.at[d, c, slot], rs_s.at[0], rs_r.at[lax.rem(c, 4), slot], z=zz(1 if d == 0 else -1))

    def rs_wait(c, slot):
        spot = rb.at[:, c, slot]
        rcopy(spot, spot, rs_s.at[0], rs_r.at[lax.rem(c, 4), slot], z=zz(1)).wait_recv()

    def first_hop(c):
        for d in range(2):
            for short in range(2):
                hf = d if short == 0 else 1 - d
                dist = 4 - short
                sb[d, c, short] = part[zz(dist if d == 0 else -dist), :, span(c, hf)].astype(bf16)
                rs_copy(d, c, 4 * short, sb.at[d, c, short]).start()

    def pass_on(c, hop, short):
        slot = 4 * short + hop - 1
        rs_wait(c, slot)
        for d in range(2):
            hf = short if d == 0 else 1 - short
            dist = 4 - hop - short
            mine = part[zz(dist if d == 0 else -dist), :, span(c, hf)]
            rb[d, c, slot] = (rb[d, c, slot].astype(f32) + mine).astype(bf16)
            rs_copy(d, c, slot + 1, rb.at[d, c, slot]).start()

    def ng_copy(c):
        at = pl.ds(pl.multiple_of(c * F, F), F)
        return pltpu.make_async_copy(ng.at[:, at], ng_o.at[:, at], ng_s.at[0])

    def finish(c):
        rs_wait(c, 3)
        rs_wait(c, 6)
        total = inner[...]
        for hf in range(2):
            at = span(c, hf)
            got = part[z, :, at] + rb[hf, c, 3].astype(f32) + rb[1 - hf, c, 6].astype(f32)
            ng[:, at] = got
            t = got * gain[:, at] * tok[z, :, at].astype(f32)
            for q in range(H // 128):
                total = total + t[:, q * 128:(q + 1) * 128]
        inner[...] = total
        ng_copy(c).start()

    def gain_part(c):
        def one(t, carry):
            per = H // 128
            at = pl.ds(pl.multiple_of(c * F + t * 128, 128), 128)
            total = jnp.zeros((rows, 128), f32)
            for b in range(Z):
                total = total + part[b, :, at] * tok[b, :, at].astype(f32) * scl[b]
            spot = pl.ds(pl.multiple_of(lax.rem(t, per) * 128, 128), 128)
            gp[c, t // per, :, spot] = jnp.sum(total, axis=0, keepdims=True)
            return carry

        lax.fori_loop(0, F // 128, one, 0)

    def gy_send(c):
        return rcopy(gp.at[c, 1 - yl], gy.at[c], gy_s.at[0], gy_r.at[0], **direct)

    def g_send(c):
        return rcopy(gp.at[c, yl], gr.at[z], g_s.at[0], g_r.at[0], z=c)

    def gf_send(k):
        return rcopy(gf.at[yl, z], gf.at[yl, z], gf_s.at[0], gf_r.at[0], z=zz(k))

    gl_copy = rcopy(gf.at[yl], gf.at[yl], gl_s.at[0], gl_r.at[0], **direct)
    g_out = [pltpu.make_async_copy(gf.at[h], gg_o.at[:, h], loc.at[10 + h]) for h in range(2)]

    def forward_quarter(t, k):
        n = jnp.where(yl == 0, t, 4 - t)
        cols = pl.ds(pl.multiple_of(n * 256, 256), 256)
        deep = dim // 4

        @pl.when(k == 0)
        def _():
            acc[...] = jnp.broadcast_to(bias[:, cols], acc.shape)

        at = pl.ds(pl.multiple_of(k * deep, deep), deep)
        lhs = nrm[:, :, at].reshape(Z * rows, deep)
        acc[...] += jnp.dot(lhs, w[at, cols], preferred_element_type=f32)

        @pl.when(k == 3)
        def _():
            for b in range(Z):
                at = pl.ds(b * rows, rows)
                for h in range(2):
                    x = acc[at, h * HEAD:(h + 1) * HEAD]
                    r = x * cosv[yl, at, :] + pltpu.roll(x, HEAD // 2, 1) * sinv[yl, at, :]
                    if h == 1:
                        r = jnp.where(n == 4, x, r)
                    out[b, :, pl.ds(pl.multiple_of(n * 256 + h * HEAD, HEAD), HEAD)] = r.astype(bf16)

    def o_copy(p):
        start = ((width, width - 128), (width + 128, 256), (width + 384, 0))[p]
        n = 128 if p == 0 else 256
        src = pl.multiple_of(jnp.where(yl == 0, start[0], start[1]), 128)
        dst = pl.multiple_of(src - (1 - yl) * width, 128)
        return rcopy(out.at[:, :, pl.ds(src, n)], qkv_o.at[:, yl, :, pl.ds(dst, n)], o_s.at[0], o_r.at[0], **direct)

    o_local = pltpu.make_async_copy(out.at[:, :, own], qkv_o.at[:, yl], loc.at[8])

    inner[...] = jnp.zeros_like(inner)

    for k in range(1, 5):
        local[k].wait()
    own_columns()
    norm_block(z)
    local[5].wait()
    bg1[...] = bgv[...].reshape(width)
    bg_copy = pltpu.make_async_copy(bg1, bg_o, loc.at[7])
    bg_copy.start()

    for k in range(PER):
        rcopy(tok.at[z], tok.at[z], ag_s.at[0], ag_r.at[k], z=zz(1)).wait_recv()
        for d in range(2):
            if k + 2 < PER:
                ag_copy(d, k + 2).start()
        for j in {1: (0, 1), 2: (2, 3), 3: (4,), 4: (5, 6), 5: (7,)}.get(k, ()):
            hand_on(j)
        for j in {3: (0, 1), 4: (2,), 6: (6,)}.get(k, ()):
            hand_over(j)
        if k == 2:
            q_copy.wait_recv()
            b_copy.wait_recv()
            bias[:, own] = b_own[...].reshape(1, width)
            bias[:, far] = b_far[...].reshape(1, width)
            far_columns()
            local[6].wait()
        if k == 5:
            for c in range(3):
                first_hop(c)
        if k in (1, 3, 5):
            norm_block(zz(-1 - k // 2))
            norm_block(zz(1 + k // 2))
        if k == 4:
            for c in range(3):
                backward_chunk(c)
            hand_over(3)
            hand_over(4)
        if k == 5:
            backward_chunk(3)
            first_hop(3)
            hand_over(5)
            backward_chunk(4)
        if k == 6:
            norm_block(zz(4))

    def event(e, carry):
        r = lax.rem(e, 16)
        base = e // 16 * 4
        hop = r // 4
        c = base + lax.rem(r, 4)

        @pl.when((hop == 0) & (e < 32))
        def _():
            first_hop(c)

        @pl.when(hop > 0)
        def _():
            j = lax.rem(r, 4)
            pair = base + 2 * lax.rem(j, 2)
            pass_on(jnp.where(hop == 2, pair, c), hop, jnp.where(hop == 2, j // 2, 0))

            @pl.when(hop < 3)
            def _():
                pass_on(jnp.where(hop == 2, pair + 1, c), hop, jnp.where(hop == 2, j // 2, 1))

        @pl.when(e == 5)
        def _():
            hand_over(7)

        @pl.when(e < 10)
        def _():
            c = 5 + (e - 4) // 2
            odd = lax.rem(e, 2)

            @pl.when(odd == 0)
            def _():
                weights_here(c)
            backward_part(c, odd * (F // bt // 2), F // bt // 2)

        @pl.when(e < 12)
        def _():
            c = e - 4
            gain_part(c)
            gy_send(c).start()

        @pl.when(e == 16)
        def _():
            rcopy(gy, gy, gy_s.at[0], gy_r.at[0], **direct).wait()
            for c in range(N):
                gp[c, yl] = gp[c, yl] + gy[c]

                @pl.when(c != z)
                def _(c=c):
                    g_send(c).start()

        @pl.when(((e >= 10) & (e < 12)) | ((e >= 16) & (e < 28)))
        def _():
            q = jnp.where(e < 12, e - 10, jnp.where(e < 22, 2 * e - 30, e - 8))
            forward_quarter(q // 4, lax.rem(q, 4))

        @pl.when((e >= 16) & (e < 22))
        def _():
            q = 2 * e - 29
            forward_quarter(q // 4, lax.rem(q, 4))

        for p, when in enumerate((20, 24, 28)):
            @pl.when(e == when)
            def _(p=p):
                o_copy(p).start()

        @pl.when(e == 21)
        def _():
            total = gp[z, yl]
            spot = gr.at[pl.ds(0, Z - 1)]
            rcopy(spot, spot, g_s.at[0], g_r.at[0], z=zz(1)).wait()
            for k in range(1, Z):
                total = total + gr[zz(k)]
            gf[yl, z] = total
            for k in range(1, Z):
                gf_send(k).start()

        @pl.when(e == 26)
        def _():
            spot = gf.at[0, pl.ds(0, Z - 1)]
            rcopy(spot, spot, gf_s.at[0], gf_r.at[0], z=zz(1)).wait()
            gl_copy.start()

        @pl.when(e == 32)
        def _():
            o_local.start()

        @pl.when(((e >= 18) & (e < 22)) | (e >= 32))
        def _():
            finish(jnp.where(e < 22, e - 18, e - 28))

        @pl.when(e == 25)
        def _():
            spot = tok.at[pl.ds(0, PER)]
            rcopy(spot, spot, ag_s.at[0], ag_r.at[0], z=zz(1)).wait_send()
            q_copy.wait_send()
            b_copy.wait_send()
            spot = w.at[:, own]
            rcopy(spot, spot, w_s.at[0], w_r.at[0], **direct).wait_send()

        @pl.when(e == 33)
        def _():
            gl_copy.wait_send()
            spot = gf.at[1 - yl]
            rcopy(spot, spot, gl_s.at[0], gl_r.at[0], **direct).wait_recv()
            for h in range(2):
                g_out[h].start()
        return carry

    lax.fori_loop(4, 36, event, 0)
    mean = jnp.sum(inner[...], axis=1, keepdims=True) / dim
    s = scl[z]
    st[0] = s
    st[1] = s * s * s * jnp.broadcast_to(mean, s.shape)
    st_copy = pltpu.make_async_copy(st, st_o, loc.at[9])
    st_copy.start()
    bg_copy.wait()
    rcopy(out.at[:, :, far], out.at[:, :, far], o_s.at[0], o_r.at[0], **direct).wait()
    rcopy(rb, rb, rs_s.at[0], rs_r.at[0, 0], z=zz(1)).wait_send()
    o_local.wait()
    for h in range(2):
        g_out[h].wait()
    pltpu.make_async_copy(ng, ng_o, ng_s.at[0]).wait()
    st_copy.wait()


def settle(
    qkv_i, ng_i, st_i, gg_i, bg_i, tok_h, gain_h, qkv_o, tg_o, gg_o, bg_o,
    qkv, ng, st, gg, bg, tok, gain, sem_i, sem_o, ng_s, tg_s,
):
    rows, dim = ng.shape
    parts = ng_s.shape[0]
    wide = dim // parts
    half = qkv.shape[0] // 2

    def loads():
        yield pltpu.make_async_copy(st_i, st, sem_i.at[0])
        yield pltpu.make_async_copy(gain_h, gain, sem_i.at[1])
        yield pltpu.make_async_copy(tok_h, tok, sem_i.at[2])

    first = list(loads())
    for copy in first:
        copy.start()
    pieces = []
    for q in range(parts):
        at = pl.ds(q * wide, wide)
        copy = pltpu.make_async_copy(ng_i.at[:, at], ng.at[:, at], ng_s.at[q])
        copy.start()
        pieces.append(copy)
    through = []
    for k, (src, mid, dst) in enumerate((
        (qkv_i.at[pl.ds(0, half)], qkv.at[pl.ds(0, half)], qkv_o.at[pl.ds(0, half)]),
        (qkv_i.at[pl.ds(half, half)], qkv.at[pl.ds(half, half)], qkv_o.at[pl.ds(half, half)]),
        (gg_i, gg, gg_o),
        (bg_i, bg, bg_o),
    )):
        copy = pltpu.make_async_copy(src, mid, sem_i.at[3 + k])
        copy.start()
        through.append((copy, pltpu.make_async_copy(mid, dst, sem_o.at[k])))
    for copy in first:
        copy.wait()
    step = 512
    s = jnp.concatenate([st[0]] * (step // 128), axis=1)
    k = jnp.concatenate([st[1]] * (step // 128), axis=1)
    sent = []
    for q in range(parts):
        pieces[q].wait()

        def one(i, carry):
            at = pl.ds(pl.multiple_of(q * wide + i * step, step), step)
            ng[:, at] = s * gain[:, at] * ng[:, at] - tok[:, at].astype(f32) * k
            return carry

        lax.fori_loop(0, wide // step, one, 0)
        at = pl.ds(q * wide, wide)
        copy = pltpu.make_async_copy(ng.at[:, at], tg_o.at[:, at], tg_s.at[q])
        copy.start()
        sent.append(copy)
        got, put = through[q]
        got.wait()
        put.start()
        sent.append(put)
    for copy in sent:
        copy.wait()


def tables(tokens_per):
    mp = 2 * Z
    block = np.arange(mp).reshape(Z, 2).T.reshape(-1)
    position = (block[:, None] * (SEQ_LEN // mp) + np.arange(tokens_per)[None, :]).reshape(-1)
    half = HEAD // 2
    inverse = np.exp(-np.log(1000000.0) * (2.0 * np.arange(half) / HEAD))
    angle = position[:, None].astype(np.float64) * inverse[None, :]
    c, s = np.cos(angle), np.sin(angle)
    shape = (2, Z * tokens_per, HEAD)
    return (
        np.concatenate([c, c], axis=1).astype(np.float32).reshape(shape),
        np.concatenate([-s, s], axis=1).astype(np.float32).reshape(shape),
    )


def shards(tokens, norm_gain, qkv_weight, qkv_bias, qkv_grad):
    rows, dim = tokens.shape
    width = qkv_weight.shape[1]
    F = dim // N
    H = F // 2
    both = 2 * width
    cos, sin = tables(rows)
    any_spec = pl.BlockSpec(memory_space=pl.ANY)
    dma = pltpu.SemaphoreType.DMA
    V = pltpu.VMEM
    raw = pl.pallas_call(
        kernel,
        name="qkv_ring",
        out_shape=(
            jax.ShapeDtypeStruct((Z, 2, rows, width), bf16),
            jax.ShapeDtypeStruct((rows, dim), f32),
            jax.ShapeDtypeStruct((2, rows, 128), f32),
            jax.ShapeDtypeStruct((Z, 2, 1, H), f32),
            jax.ShapeDtypeStruct((width,), f32),
        ),
        in_specs=[any_spec] * 7,
        out_specs=(any_spec,) * 5,
        scratch_shapes=[
            V((dim, both), bf16),
            V((Z, rows, dim), bf16),
            V((Z, rows, dim), bf16),
            V((Z, rows, dim), f32),
            V((2, N, PER, rows, H), bf16),
            V((2, N, 2, rows, H), bf16),
            V((Z, 2, rows, width), bf16),
            V((Z, rows, width), bf16),
            V((Z * rows, both), bf16),
            V((Z, rows, both), bf16),
            V((rows, dim), f32),
            V((2, rows, 128), f32),
            V((Z, rows, 128), f32),
            V((rows, 128), f32),
            V((Z * rows, 256), f32),
            V((N, 2, 1, H), f32),
            V((Z, 1, H), f32),
            V((N, 1, H), f32),
            V((2, Z, 1, H), f32),
            V((1, dim), f32),
            V((1, both), f32),
            V((width,), f32),
            V((width,), f32),
            V((1, width), f32),
            V((width,), f32),
            V(cos.shape, f32),
            V(sin.shape, f32),
            dma((PER,)), dma((1,)),
            dma((N,)), dma((1,)), dma((N,)), dma((N,)),
            dma((4, PER)), dma((1,)),
            dma((1,)), dma((1,)),
            dma((1,)), dma((1,)),
            dma((1,)), dma((1,)),
            dma((1,)), dma((1,)),
            dma((1,)), dma((1,)),
            dma((1,)), dma((1,)),
            dma((1,)), dma((1,)),
            dma((1,)),
            dma((14,)),
        ],
        compiler_params=pltpu.CompilerParams(
            collective_id=0, has_side_effects=True, vmem_limit_bytes=66_000_000
        ),
    )(
        tokens,
        qkv_weight,
        qkv_grad.reshape(Z, 2, rows, width),
        norm_gain.reshape(1, dim),
        qkv_bias,
        jnp.asarray(cos),
        jnp.asarray(sin),
    )
    qkv, tokens_grad, gain_grad, bias_grad = pl.pallas_call(
        settle,
        name="settle",
        out_shape=(
            jax.ShapeDtypeStruct((Z, 2, rows, width), bf16),
            jax.ShapeDtypeStruct((rows, dim), f32),
            jax.ShapeDtypeStruct((Z, 2, 1, H), f32),
            jax.ShapeDtypeStruct((width,), f32),
        ),
        in_specs=[any_spec] * 7,
        out_specs=(any_spec,) * 4,
        scratch_shapes=[
            V((Z, 2, rows, width), bf16),
            V((rows, dim), f32),
            V((2, rows, 128), f32),
            V((Z, 2, 1, H), f32),
            V((width,), f32),
            V((rows, dim), bf16),
            V((1, dim), f32),
            dma((7,)), dma((4,)), dma((4,)), dma((4,)),
        ],
        compiler_params=pltpu.CompilerParams(vmem_limit_bytes=66_000_000),
    )(*raw, tokens, norm_gain.reshape(1, dim))
    return (
        qkv.reshape(2 * Z * rows, width),
        tokens_grad,
        gain_grad.reshape(dim),
        bias_grad,
    )


def solution(mesh):
    dp, mp = AXES[:3], AXES[3:]
    split = Mesh(mesh.devices.reshape(2, mesh.shape["dp"] // 4, 2, Z, 2), AXES)
    return jax.shard_map(
        shards,
        mesh=split,
        in_specs=(P(AXES, None), P(), P(None, mp), P(mp), P(dp, mp)),
        out_specs=(P(dp, mp), P(AXES, None), P(dp), P(AXES)),
        check_vma=False,
    )
```

```python
import functools

import jax
import jax.numpy as jnp
import numpy as np
from jax import lax
from jax.experimental import pallas as pl
from jax.experimental.pallas import tpu as pltpu
from jax.sharding import Mesh
from jax.sharding import PartitionSpec as P

HEAD = 128
SEQ_LEN = 32768
MESH = pl.DeviceIdType.MESH
AXES = ("yh", "x", "core", "z", "yl")
Z = 8
N = 8
PER = 7
f32 = jnp.float32
bf16 = jnp.bfloat16


def rcopy(src, dst, ssem, rsem, **where):
    return pltpu.make_async_remote_copy(
        src_ref=src, dst_ref=dst, send_sem=ssem, recv_sem=rsem, device_id=where, device_id_type=MESH
    )


def kernel(
    tok_h, w_h, qg_h, gain_h, bias_h, cos_h, sin_h,
    qkv_o, ng_o, st_o, gg_o, bg_o,
    w, tok, nrm, part, rb, sb, qb, qp, jl, out, ng, st, scl, inner, acc,
    gp, gr, gy, gf, gain, bias, b_own, b_far, bgv, bg1, cosv, sinv,
    ag_r, ag_s, w_r, w_s, x_r, d_r, rs_r, rs_s, q_r, q_s, b_r, b_s, o_r, o_s,
    g_r, g_s, gy_r, gy_s, gf_r, gf_s, gl_r, gl_s, ng_s, loc,
):
    rows, dim = tok_h.shape
    width = w_h.shape[1]
    F = dim // N
    H = F // 2
    half = dim // 2
    yh, x, core, z, yl = (lax.axis_index(a) for a in AXES)

    def zz(k):
        return lax.rem(z + (k + Z), Z)

    direct = {"yl": 1 - yl}
    other = {"yh": 1 - yh, "yl": 1 - yl}
    sibling = {"core": 1 - core}
    nx = lax.axis_size("x")
    beside = [{"x": lax.rem(x + 1, nx)}, {"x": lax.rem(x + nx - 1, nx)}]
    side = lax.rem(x, 2)
    own = pl.ds(pl.multiple_of(yl * width, 128), width)
    far = pl.ds(pl.multiple_of((1 - yl) * width, 128), width)

    local = [
        pltpu.make_async_copy(tok_h, tok.at[z], loc.at[0]),
        pltpu.make_async_copy(qg_h, qb, loc.at[1]),
        pltpu.make_async_copy(cos_h, cosv, loc.at[2]),
        pltpu.make_async_copy(sin_h, sinv, loc.at[3]),
        pltpu.make_async_copy(gain_h, gain, loc.at[4]),
        pltpu.make_async_copy(bias_h, b_own, loc.at[5]),
        pltpu.make_async_copy(w_h, w.at[:, own], loc.at[6]),
    ]
    for copy in local:
        copy.start()

    barrier = pltpu.get_barrier_semaphore()
    for where in ({"z": zz(1)}, {"z": zz(-1)}, direct, other, sibling, *beside):
        pl.semaphore_signal(barrier, inc=1, device_id=where, device_id_type=MESH)
    pl.semaphore_wait(barrier, 7)
    local[0].wait()

    def ag_half(d, k):
        return d if k % 2 == 0 else 1 - d

    def ag_copy(d, k):
        step = k // 2
        block = zz(-step) if d == 0 else zz(step)
        cols = pl.ds(ag_half(d, k) * half, half)
        spot = tok.at[block, :, cols]
        return rcopy(spot, spot, ag_s.at[0], ag_r.at[k], z=zz(1 if d == 0 else -1))

    for k in range(2):
        for d in range(2):
            ag_copy(d, k).start()

    q_copy = rcopy(qg_h.at[:, 1 - yl], qp, q_s.at[0], q_r.at[0], **direct)
    b_copy = rcopy(bias_h, b_far, b_s.at[0], b_r.at[0], **direct)

    piece = F // 8

    cut = 7 * piece // 8

    def w_rows(j, par, who, s, n):
        first = j * F + par * 4 * piece + who * 2 * piece
        if n > 1:
            return pl.ds(pl.multiple_of(first, 2 * piece), n * piece)
        return pl.ds(pl.multiple_of(first + s * cut, 16), cut if s == 0 else 2 * piece - cut)

    def w_copy(j, s):
        at = w_rows(j, side, core, s, 1)
        return rcopy(w_h.at[at], w.at[at, own], w_s.at[0], w_r.at[j], **(direct if s == 0 else other))

    def w_got(j):
        spot = w.at[w_rows(j, side, core, 0, 2), far]
        return rcopy(spot, spot, w_s.at[0], w_r.at[j], **direct)

    def x_copy(j, s):
        spot = w.at[w_rows(j, side, core, 0, 2), far].at[pl.ds(s * piece, piece)]
        return rcopy(spot, spot, w_s.at[0], x_r.at[j], **beside[s])

    def x_got(j):
        spot = w.at[w_rows(j, 1 - side, core, 0, 2), far]
        return rcopy(spot, spot, w_s.at[0], x_r.at[j], **beside[0])

    def d_copy(j, k):
        spot = w.at[w_rows(j, side if k == 0 else 1 - side, core, 0, 2), far]
        return rcopy(spot, spot, w_s.at[0], d_r.at[j], **sibling)

    def hand_on(j):
        w_got(j).wait_recv()
        for s in range(2):
            x_copy(j, s).start()
        d_copy(j, 0).start()

    def hand_over(j):
        x_got(j).wait_recv()
        d_copy(j, 1).start()

    for j in range(N):
        if j == 4:
            b_copy.start()
            q_copy.start()
        w_copy(j, 0).start()
        w_copy(j, 1).start()

    def norm_block(b):
        step = min(512, dim)

        def sq(i, total):
            v = tok[b, :, pl.ds(pl.multiple_of(i * step, step), step)].astype(f32)
            v = v * v
            for q in range(step // 128):
                total = total + v[:, q * 128:(q + 1) * 128]
            return total

        total = lax.fori_loop(0, dim // step, sq, jnp.zeros((rows, 128), f32))
        mean = jnp.sum(total, axis=1, keepdims=True) / dim
        s = jnp.broadcast_to(lax.rsqrt(mean + 1e-06), (rows, 128))
        scl[b] = s
        wide = jnp.concatenate([s] * (step // 128), axis=1)

        def put(i, carry):
            at = pl.ds(pl.multiple_of(i * step, step), step)
            v = tok[b, :, at].astype(f32)
            nrm[b, :, at] = (v * wide * gain[:, at]).astype(bf16)
            return carry

        lax.fori_loop(0, dim // step, put, 0)

    def turn_back(x, line, b, is_value):
        c = cosv[line, pl.ds(pl.multiple_of(b * rows, rows), rows), :]
        s = sinv[line, pl.ds(pl.multiple_of(b * rows, rows), rows), :]
        r = x * c - pltpu.roll(x, HEAD // 2, 1) * s
        return r if is_value is None else jnp.where(is_value, x, r)

    heads = width // HEAD

    def own_columns():
        def one(b, sums):
            at = pl.ds(pl.multiple_of(b * rows, rows), rows)
            new = []
            for h in range(heads):
                value = (yl == 1) if h == heads - 1 else None
                hs = pl.ds(h * HEAD, HEAD)
                r = turn_back(qb[b, yl, :, hs].astype(f32), yl, b, value)
                jl[at, pl.ds(pl.multiple_of(yl * width + h * HEAD, HEAD), HEAD)] = r.astype(bf16)
                r = r + turn_back(qb[b, 1 - yl, :, hs].astype(f32), 1 - yl, b, value)
                total = sums[h]
                for q in range(rows // 8):
                    total = total + r[q * 8:(q + 1) * 8]
                new.append(total)
            return tuple(new)

        sums = lax.fori_loop(0, Z, one, (jnp.zeros((8, HEAD), f32),) * heads)
        for h in range(heads):
            bgv[:, h * HEAD:(h + 1) * HEAD] = jnp.sum(sums[h], axis=0, keepdims=True)

    def far_columns():
        def one(b, carry):
            at = pl.ds(pl.multiple_of(b * rows, rows), rows)
            for h in range(heads):
                value = (yl == 0) if h == heads - 1 else None
                r = turn_back(qp[b, :, pl.ds(h * HEAD, HEAD)].astype(f32), yl, b, value)
                jl[at, pl.ds(pl.multiple_of((1 - yl) * width + h * HEAD, HEAD), HEAD)] = r.astype(bf16)
            return carry

        lax.fori_loop(0, Z, one, 0)

    bt = min(256, F)

    def backward_part(c, first, count):
        def one(t, carry):
            at = pl.ds(pl.multiple_of(c * F + t * bt, bt), bt)
            got = lax.dot_general(jl[...], w[at, :], (((1,), (1,)), ((), ())), preferred_element_type=f32)
            part[:, :, at] = got.reshape(Z, rows, bt)
            return carry

        lax.fori_loop(first, first + count, one, 0)

    def weights_here(c):
        spot = w.at[w_rows(c, 0, 0, 0, 4), far]
        rcopy(spot, spot, w_s.at[0], d_r.at[c], **sibling).wait_recv()

    def backward_chunk(c):
        weights_here(c)
        backward_part(c, 0, F // bt)

    def span(c, hf):
        return pl.ds(pl.multiple_of(c * F + hf * H, H), H)

    def rs_copy(d, c, slot, src):
        got = jnp.where(slot == 6, 3, slot)
        return rcopy(src, rb.at[d, c, slot], rs_s.at[0], rs_r.at[lax.rem(c, 4), got], z=zz(1 if d == 0 else -1))

    def rs_wait(c, slot):
        spot = rb.at[:, c, slot]
        rcopy(spot, spot, rs_s.at[0], rs_r.at[lax.rem(c, 4), slot], z=zz(1)).wait_recv()

    def first_hop(c):
        for d in range(2):
            for short in range(2):
                hf = d if short == 0 else 1 - d
                dist = 4 - short
                sb[d, c, short] = part[zz(dist if d == 0 else -dist), :, span(c, hf)].astype(bf16)
                rs_copy(d, c, 4 * short, sb.at[d, c, short]).start()

    def pass_on(c, hop, short):
        slot = 4 * short + hop - 1
        rs_wait(c, slot)
        for d in range(2):
            hf = short if d == 0 else 1 - short
            dist = 4 - hop - short
            mine = part[zz(dist if d == 0 else -dist), :, span(c, hf)]
            rb[d, c, slot] = (rb[d, c, slot].astype(f32) + mine).astype(bf16)
            rs_copy(d, c, slot + 1, rb.at[d, c, slot]).start()

    def ng_copy(c):
        at = pl.ds(pl.multiple_of(c * F, F), F)
        return pltpu.make_async_copy(ng.at[:, at], ng_o.at[:, at], ng_s.at[0])

    def finish(c):
        spot = rb.at[:, c, pl.ds(3, 2)]
        rcopy(spot, spot, rs_s.at[0], rs_r.at[lax.rem(c, 4), 3], z=zz(1)).wait_recv()
        total = inner[...]
        for hf in range(2):
            at = span(c, hf)
            got = part[z, :, at] + rb[hf, c, 3].astype(f32) + rb[1 - hf, c, 6].astype(f32)
            ng[:, at] = got
            t = got * gain[:, at] * tok[z, :, at].astype(f32)
            for q in range(H // 128):
                total = total + t[:, q * 128:(q + 1) * 128]
        inner[...] = total
        ng_copy(c).start()

    def gain_part(c):
        def one(t, carry):
            per = H // 128
            at = pl.ds(pl.multiple_of(c * F + t * 128, 128), 128)
            total = jnp.zeros((rows, 128), f32)
            for b in range(Z):
                total = total + part[b, :, at] * tok[b, :, at].astype(f32) * scl[b]
            spot = pl.ds(pl.multiple_of(lax.rem(t, per) * 128, 128), 128)
            gp[c, t // per, :, spot] = jnp.sum(total, axis=0, keepdims=True)
            return carry

        lax.fori_loop(0, F // 128, one, 0)

    def gy_send(c):
        return rcopy(gp.at[c, 1 - yl], gy.at[c], gy_s.at[0], gy_r.at[0], **direct)

    def g_send(c):
        return rcopy(gp.at[c, yl], gr.at[z], g_s.at[0], g_r.at[0], z=c)

    def gf_send(k):
        return rcopy(gf.at[yl, z], gf.at[yl, z], gf_s.at[0], gf_r.at[0], z=zz(k))

    gl_copy = rcopy(gf.at[yl], gf.at[yl], gl_s.at[0], gl_r.at[0], **direct)
    g_out = [pltpu.make_async_copy(gf.at[h], gg_o.at[:, h], loc.at[10 + h]) for h in range(2)]

    def forward_quarter(t, k):
        n = jnp.where(yl == 0, t, 4 - t)
        cols = pl.ds(pl.multiple_of(n * 256, 256), 256)
        deep = dim // 4

        @pl.when(k == 0)
        def _():
            acc[...] = jnp.broadcast_to(bias[:, cols], acc.shape)

        at = pl.ds(pl.multiple_of(k * deep, deep), deep)
        lhs = nrm[:, :, at].reshape(Z * rows, deep)
        acc[...] += jnp.dot(lhs, w[at, cols], preferred_element_type=f32)

        @pl.when(k == 3)
        def _():
            for b in range(Z):
                at = pl.ds(b * rows, rows)
                for h in range(2):
                    x = acc[at, h * HEAD:(h + 1) * HEAD]
                    r = x * cosv[yl, at, :] + pltpu.roll(x, HEAD // 2, 1) * sinv[yl, at, :]
                    if h == 1:
                        r = jnp.where(n == 4, x, r)
                    out[b, :, pl.ds(pl.multiple_of(n * 256 + h * HEAD, HEAD), HEAD)] = r.astype(bf16)

    def o_copy(p):
        start = ((width, width - 128), (width + 128, 256), (width + 384, 0))[p]
        n = 128 if p == 0 else 256
        src = pl.multiple_of(jnp.where(yl == 0, start[0], start[1]), 128)
        dst = pl.multiple_of(src - (1 - yl) * width, 128)
        return rcopy(out.at[:, :, pl.ds(src, n)], qkv_o.at[:, yl, :, pl.ds(dst, n)], o_s.at[0], o_r.at[0], **direct)

    o_local = pltpu.make_async_copy(out.at[:, :, own], qkv_o.at[:, yl], loc.at[8])

    inner[...] = jnp.zeros_like(inner)

    for k in range(1, 5):
        local[k].wait()
    own_columns()
    norm_block(z)
    local[5].wait()
    bg1[...] = bgv[...].reshape(width)
    bg_copy = pltpu.make_async_copy(bg1, bg_o, loc.at[7])
    bg_copy.start()

    for k in range(PER):
        rcopy(tok.at[z], tok.at[z], ag_s.at[0], ag_r.at[k], z=zz(1)).wait_recv()
        for d in range(2):
            if k + 2 < PER:
                ag_copy(d, k + 2).start()
        for j in {1: (0, 1), 2: (2, 3), 3: (4,), 4: (5, 6), 5: (7,)}.get(k, ()):
            hand_on(j)
        for j in {3: (0, 1), 4: (2,), 6: (6,)}.get(k, ()):
            hand_over(j)
        if k == 2:
            q_copy.wait_recv()
            b_copy.wait_recv()
            bias[:, own] = b_own[...].reshape(1, width)
            bias[:, far] = b_far[...].reshape(1, width)
            far_columns()
            local[6].wait()
        if k == 5:
            for c in range(3):
                first_hop(c)
        if k in (1, 3, 5):
            norm_block(zz(-1 - k // 2))
            norm_block(zz(1 + k // 2))
        if k == 4:
            for c in range(3):
                backward_chunk(c)
            hand_over(3)
            hand_over(4)
        if k == 5:
            backward_chunk(3)
            first_hop(3)
            hand_over(5)
            backward_chunk(4)
        if k == 6:
            norm_block(zz(4))

    def event(e, carry):
        r = lax.rem(e, 16)
        base = e // 16 * 4
        hop = r // 4
        c = base + lax.rem(r, 4)

        @pl.when((hop == 0) & (e < 32))
        def _():
            first_hop(c)

        @pl.when(hop > 0)
        def _():
            j = lax.rem(r, 4)
            pair = base + 2 * lax.rem(j, 2)
            pass_on(jnp.where(hop == 2, pair, c), hop, jnp.where(hop == 2, j // 2, 0))

            @pl.when(hop < 3)
            def _():
                pass_on(jnp.where(hop == 2, pair + 1, c), hop, jnp.where(hop == 2, j // 2, 1))

        @pl.when(e == 5)
        def _():
            hand_over(7)

        @pl.when(e < 10)
        def _():
            c = 5 + (e - 4) // 2
            odd = lax.rem(e, 2)

            @pl.when(odd == 0)
            def _():
                weights_here(c)
            backward_part(c, odd * (F // bt // 2), F // bt // 2)

        @pl.when(e < 12)
        def _():
            c = e - 4
            gain_part(c)
            gy_send(c).start()

        @pl.when(e == 16)
        def _():
            rcopy(gy, gy, gy_s.at[0], gy_r.at[0], **direct).wait()
            for c in range(N):
                gp[c, yl] = gp[c, yl] + gy[c]

                @pl.when(c != z)
                def _(c=c):
                    g_send(c).start()

        @pl.when(((e >= 10) & (e < 12)) | ((e >= 16) & (e < 28)))
        def _():
            q = jnp.where(e < 12, e - 10, jnp.where(e < 22, 2 * e - 30, e - 8))
            forward_quarter(q // 4, lax.rem(q, 4))

        @pl.when((e >= 16) & (e < 22))
        def _():
            q = 2 * e - 29
            forward_quarter(q // 4, lax.rem(q, 4))

        for p, when in enumerate((20, 24, 28)):
            @pl.when(e == when)
            def _(p=p):
                o_copy(p).start()

        @pl.when(e == 21)
        def _():
            total = gp[z, yl]
            spot = gr.at[pl.ds(0, Z - 1)]
            rcopy(spot, spot, g_s.at[0], g_r.at[0], z=zz(1)).wait()
            for k in range(1, Z):
                total = total + gr[zz(k)]
            gf[yl, z] = total
            for k in range(1, Z):
                gf_send(k).start()

        @pl.when(e == 26)
        def _():
            spot = gf.at[0, pl.ds(0, Z - 1)]
            rcopy(spot, spot, gf_s.at[0], gf_r.at[0], z=zz(1)).wait()
            gl_copy.start()

        @pl.when(e == 32)
        def _():
            o_local.start()

        @pl.when(((e >= 18) & (e < 22)) | (e >= 32))
        def _():
            finish(jnp.where(e < 22, e - 18, e - 28))

        @pl.when(e == 25)
        def _():
            spot = tok.at[pl.ds(0, PER)]
            rcopy(spot, spot, ag_s.at[0], ag_r.at[0], z=zz(1)).wait_send()
            q_copy.wait_send()
            b_copy.wait_send()
            spot = w.at[:, own]
            rcopy(spot, spot, w_s.at[0], w_r.at[0], **direct).wait_send()

        @pl.when(e == 33)
        def _():
            gl_copy.wait_send()
            spot = gf.at[1 - yl]
            rcopy(spot, spot, gl_s.at[0], gl_r.at[0], **direct).wait_recv()
            for h in range(2):
                g_out[h].start()
        return carry

    lax.fori_loop(4, 36, event, 0)
    mean = jnp.sum(inner[...], axis=1, keepdims=True) / dim
    s = scl[z]
    st[0] = s
    st[1] = s * s * s * jnp.broadcast_to(mean, s.shape)
    st_copy = pltpu.make_async_copy(st, st_o, loc.at[9])
    st_copy.start()
    bg_copy.wait()
    rcopy(out.at[:, :, far], out.at[:, :, far], o_s.at[0], o_r.at[0], **direct).wait()
    rcopy(rb, rb, rs_s.at[0], rs_r.at[0, 0], z=zz(1)).wait_send()
    o_local.wait()
    for h in range(2):
        g_out[h].wait()
    pltpu.make_async_copy(ng, ng_o, ng_s.at[0]).wait()
    st_copy.wait()


def settle(
    qkv_i, ng_i, st_i, gg_i, bg_i, tok_h, gain_h, qkv_o, tg_o, gg_o, bg_o,
    qkv, ng, st, gg, bg, tok, gain, sem_i, sem_o, ng_s, tg_s,
):
    rows, dim = ng.shape
    parts = ng_s.shape[0]
    wide = dim // parts
    half = qkv.shape[0] // 2

    def loads():
        yield pltpu.make_async_copy(st_i, st, sem_i.at[0])
        yield pltpu.make_async_copy(gain_h, gain, sem_i.at[1])
        yield pltpu.make_async_copy(tok_h, tok, sem_i.at[2])

    first = list(loads())
    for copy in first:
        copy.start()
    pieces = []
    for q in range(parts):
        at = pl.ds(q * wide, wide)
        copy = pltpu.make_async_copy(ng_i.at[:, at], ng.at[:, at], ng_s.at[q])
        copy.start()
        pieces.append(copy)
    through = []
    for k, (src, mid, dst) in enumerate((
        (qkv_i.at[pl.ds(0, half)], qkv.at[pl.ds(0, half)], qkv_o.at[pl.ds(0, half)]),
        (qkv_i.at[pl.ds(half, half)], qkv.at[pl.ds(half, half)], qkv_o.at[pl.ds(half, half)]),
        (gg_i, gg, gg_o),
        (bg_i, bg, bg_o),
    )):
        copy = pltpu.make_async_copy(src, mid, sem_i.at[3 + k])
        copy.start()
        through.append((copy, pltpu.make_async_copy(mid, dst, sem_o.at[k])))
    for copy in first:
        copy.wait()
    step = 512
    s = jnp.concatenate([st[0]] * (step // 128), axis=1)
    k = jnp.concatenate([st[1]] * (step // 128), axis=1)
    sent = []
    for q in range(parts):
        pieces[q].wait()

        def one(i, carry):
            at = pl.ds(pl.multiple_of(q * wide + i * step, step), step)
            ng[:, at] = s * gain[:, at] * ng[:, at] - tok[:, at].astype(f32) * k
            return carry

        lax.fori_loop(0, wide // step, one, 0)
        at = pl.ds(q * wide, wide)
        copy = pltpu.make_async_copy(ng.at[:, at], tg_o.at[:, at], tg_s.at[0])
        copy.start()
        got, put = through[q]
        got.wait()
        put.start()
        sent.append(put)
    for copy in sent:
        copy.wait()
    pltpu.make_async_copy(ng, tg_o, tg_s.at[0]).wait()


def tables(tokens_per):
    mp = 2 * Z
    block = np.arange(mp).reshape(Z, 2).T.reshape(-1)
    position = (block[:, None] * (SEQ_LEN // mp) + np.arange(tokens_per)[None, :]).reshape(-1)
    half = HEAD // 2
    inverse = np.exp(-np.log(1000000.0) * (2.0 * np.arange(half) / HEAD))
    angle = position[:, None].astype(np.float64) * inverse[None, :]
    c, s = np.cos(angle), np.sin(angle)
    shape = (2, Z * tokens_per, HEAD)
    return (
        np.concatenate([c, c], axis=1).astype(np.float32).reshape(shape),
        np.concatenate([-s, s], axis=1).astype(np.float32).reshape(shape),
    )


def shards(tokens, norm_gain, qkv_weight, qkv_bias, qkv_grad):
    rows, dim = tokens.shape
    width = qkv_weight.shape[1]
    F = dim // N
    H = F // 2
    both = 2 * width
    cos, sin = tables(rows)
    any_spec = pl.BlockSpec(memory_space=pl.ANY)
    dma = pltpu.SemaphoreType.DMA
    V = pltpu.VMEM
    raw = pl.pallas_call(
        kernel,
        name="qkv_ring",
        out_shape=(
            jax.ShapeDtypeStruct((Z, 2, rows, width), bf16),
            jax.ShapeDtypeStruct((rows, dim), f32),
            jax.ShapeDtypeStruct((2, rows, 128), f32),
            jax.ShapeDtypeStruct((Z, 2, 1, H), f32),
            jax.ShapeDtypeStruct((width,), f32),
        ),
        in_specs=[any_spec] * 7,
        out_specs=(any_spec,) * 5,
        scratch_shapes=[
            V((dim, both), bf16),
            V((Z, rows, dim), bf16),
            V((Z, rows, dim), bf16),
            V((Z, rows, dim), f32),
            V((2, N, PER, rows, H), bf16),
            V((2, N, 2, rows, H), bf16),
            V((Z, 2, rows, width), bf16),
            V((Z, rows, width), bf16),
            V((Z * rows, both), bf16),
            V((Z, rows, both), bf16),
            V((rows, dim), f32),
            V((2, rows, 128), f32),
            V((Z, rows, 128), f32),
            V((rows, 128), f32),
            V((Z * rows, 256), f32),
            V((N, 2, 1, H), f32),
            V((Z, 1, H), f32),
            V((N, 1, H), f32),
            V((2, Z, 1, H), f32),
            V((1, dim), f32),
            V((1, both), f32),
            V((width,), f32),
            V((width,), f32),
            V((1, width), f32),
            V((width,), f32),
            V(cos.shape, f32),
            V(sin.shape, f32),
            dma((PER,)), dma((1,)),
            dma((N,)), dma((1,)), dma((N,)), dma((N,)),
            dma((4, PER - 1)), dma((1,)),
            dma((1,)), dma((1,)),
            dma((1,)), dma((1,)),
            dma((1,)), dma((1,)),
            dma((1,)), dma((1,)),
            dma((1,)), dma((1,)),
            dma((1,)), dma((1,)),
            dma((1,)), dma((1,)),
            dma((1,)),
            dma((12,)),
        ],
        compiler_params=pltpu.CompilerParams(
            collective_id=0, has_side_effects=True, vmem_limit_bytes=66_000_000
        ),
    )(
        tokens,
        qkv_weight,
        qkv_grad.reshape(Z, 2, rows, width),
        norm_gain.reshape(1, dim),
        qkv_bias,
        jnp.asarray(cos),
        jnp.asarray(sin),
    )
    qkv, tokens_grad, gain_grad, bias_grad = pl.pallas_call(
        settle,
        name="settle",
        out_shape=(
            jax.ShapeDtypeStruct((Z, 2, rows, width), bf16),
            jax.ShapeDtypeStruct((rows, dim), f32),
            jax.ShapeDtypeStruct((Z, 2, 1, H), f32),
            jax.ShapeDtypeStruct((width,), f32),
        ),
        in_specs=[any_spec] * 7,
        out_specs=(any_spec,) * 4,
        scratch_shapes=[
            V((Z, 2, rows, width), bf16),
            V((rows, dim), f32),
            V((2, rows, 128), f32),
            V((Z, 2, 1, H), f32),
            V((width,), f32),
            V((rows, dim), bf16),
            V((1, dim), f32),
            dma((7,)), dma((4,)), dma((4,)), dma((1,)),
        ],
        compiler_params=pltpu.CompilerParams(vmem_limit_bytes=66_000_000),
    )(*raw, tokens, norm_gain.reshape(1, dim))
    return (
        qkv.reshape(2 * Z * rows, width),
        tokens_grad,
        gain_grad.reshape(dim),
        bias_grad,
    )


def solution(mesh):
    dp, mp = AXES[:3], AXES[3:]
    split = Mesh(mesh.devices.reshape(2, mesh.shape["dp"] // 4, 2, Z, 2), AXES)
    return jax.shard_map(
        shards,
        mesh=split,
        in_specs=(P(AXES, None), P(), P(None, mp), P(mp), P(dp, mp)),
        out_specs=(P(dp, mp), P(AXES, None), P(dp), P(AXES)),
        check_vma=False,
    )
```
